32 devices in a mesh: groups: 2 (over y), center: 8 (over z, x), row: 2 (over core).
Axes of the slice: x: 2, y: 2, z: 4, core: 2. Of those that a mesh axis runs over, the one named last changes fastest.
Arguments:
- dataset: float32 [512, 1024], P(('groups', 'center', 'row')), parts along dimension 0, may hold values from -0.1875 to 0.1875
- centers: float32 [2048, 1024], P(('groups', 'center')), parts along dimension 0, may hold values from -0.1875 to 0.1875
- weights: float32 [2048, 512], P(('groups', 'center'), 'row'), parts along dimension 0, may hold values from -0.1875 to 0.1875
- batch_index: int32 [2, 128], P(None, ('groups', 'center', 'row')), parts along dimension 1, may hold values from 0 to 15
- targets: float32 [2, 128, 512], P(None, ('groups', 'center', 'row')), parts along dimension 1, may hold values from -6 to 6
- gamma: float32 [2], P('groups'), parts along dimension 0, may hold values from 0.3 to 1.5
Outputs:
- new_weights: float32 [2048, 512], P(('groups', 'center'), 'row'), parts along dimension 0
- residual: float32 [128, 512], P(('groups', 'center', 'row')), parts along dimension 0
The draws below stay inside these ranges and needn't reach their ends.
There are 2 independent parts, one for each index of `groups`. The reference program is written for one: setup_inputs(seed, part) draws one part's arguments, and reference() takes and returns one part's arrays. A program takes and returns all parts, laid end to end along the dimension named above; each array names one. Nothing has to cross between parts.
Inputs may be any that keep to these rules, and one draw needn't show every extreme that they name: `batch_index`: each entry picks a row within the block of 16 dataset rows that has the same block number as the entry's block of 4 batch rows.
All inputs are finite; a program needn't handle non-finite values.
Results may differ from the reference program's by a relative error of at most 0.0001.
Values sent between devices are 32-bit elements; how exact they have to be, the bound alone decides.
No kernel may reach another device: no remote copies, remote signals or barrier semaphores. Data moves between devices by JAX's collectives and lax.ppermute only.
A program may use at most 64 MiB of HBM per device.

```python
import math
import jax
import jax.numpy as jnp
from jax import lax

F = 1024
K = 512
ROWS_DEV = 4
DATA_DEV = 16
CENTERS = 1024
BATCH = 64
NDATA = 256
N_CENTER = 8
N_ROW = 2


def shared_centroids(key):
    centroid = jax.random.normal(jax.random.fold_in(key, 5), (64, F), jnp.float32) * F ** (-0.5)
    return centroid


def clustered(key, amount, seed_tag):
    centroid = shared_centroids(key)
    member = jax.random.randint(jax.random.fold_in(key, seed_tag), (amount,), 0, 64)
    chosen = centroid[member]
    jitter = jax.random.normal(jax.random.fold_in(key, seed_tag + 1), (amount, F), jnp.float32)
    points = chosen + jitter * (0.5 * F ** (-0.5))
    return jnp.clip(points, -6.0 * F ** (-0.5), 6.0 * F ** (-0.5))


def draw_dataset(key, part):
    return clustered(key, NDATA, 21)


def draw_centers(key, part):
    return clustered(key, CENTERS, 31)


def touch_ends(entries, own_key, least, top_value):
    longest = entries.shape.index(max(entries.shape))
    spots = []
    for shift in (0, 1):
        where = [jax.random.randint(jax.random.fold_in(own_key, axis), (), 0, length) for axis, length in enumerate(entries.shape)]
        where[longest] = (where[longest] + shift) % entries.shape[longest]
        spots.append(tuple(where))
    return entries.at[spots[0]].set(least).at[spots[1]].set(top_value)


def steps_of(stream_key, extent, split, least, top_value):
    def one(position, blocks):
        heights = jax.random.uniform(jax.random.fold_in(jax.random.fold_in(stream_key, 6), position), (blocks,), jnp.float32, least / len(split), top_value / len(split))
        return jnp.repeat(jnp.exp(heights), extent[position] // blocks).reshape((-1,) + (1,) * (len(extent) - position - 1))

    factor_of = one(*split[0])
    for cut in split[1:]:
        factor_of = factor_of * one(*cut)
    return factor_of


def noise(own_key, extent, width, most, shards=(), held_as=jnp.bfloat16):
    result = width * jax.random.normal(own_key, extent, jnp.float32)
    if shards:
        result = result * steps_of(own_key, extent, shards, -0.22, 0.18)
    return jnp.clip(result, -most, most).astype(held_as)


def setup_inputs(seed: int = 0, part: int = 0) -> dict:
    key_of = jax.random.split(jax.random.key(seed), 7)
    part_keys = jax.random.split(jax.random.fold_in(key_of[6], part), 7)
    return {
        "dataset": draw_dataset(jax.random.fold_in(jax.random.fold_in(key_of[6], part), 71), part),
        "centers": draw_centers(jax.random.fold_in(jax.random.fold_in(key_of[6], part), 71), part),
        "weights": noise(part_keys[2], (CENTERS, K), CENTERS ** -0.5, 0.1875, ((0, 8), (1, 2)), jnp.float32),
        "batch_index": touch_ends(jax.random.randint(part_keys[3], (2, BATCH), 0, DATA_DEV), jax.random.fold_in(part_keys[3], 1), 0, DATA_DEV - 1).astype(jnp.int32),
        "targets": noise(part_keys[4], (2, BATCH, K), 1.0, 6.0, ((1, 16),), jnp.float32),
        "gamma": jnp.clip(jnp.exp(jax.random.uniform(part_keys[5], (1,), jnp.float32, math.log(0.3), math.log(1.5))), 0.3, 1.5),
    }


def reference(dataset, centers, weights, batch_index, targets, gamma):
    blocks = N_CENTER * N_ROW
    grouped = dataset.reshape(blocks, DATA_DEV, F)
    center_sq = jnp.sum(centers * centers, axis=1)
    current = weights
    residual = None
    for step in range(2):
        picks = batch_index[step].reshape(blocks, ROWS_DEV)
        rows = jnp.take_along_axis(grouped, picks[:, :, None], axis=1).reshape(BATCH, F)
        row_sq = jnp.sum(rows * rows, axis=1)
        cross = jnp.dot(rows, centers.T, precision=lax.Precision.HIGHEST, preferred_element_type=jnp.float32)
        kernel = jnp.exp(-gamma[0] * (row_sq[:, None] + center_sq[None, :] - 2.0 * cross))
        predict = jnp.dot(kernel, current, precision=lax.Precision.HIGHEST, preferred_element_type=jnp.float32)
        residual = predict - targets[step]
        grad = jnp.dot(kernel.T, residual, precision=lax.Precision.HIGHEST, preferred_element_type=jnp.float32)
        current = current - (0.5 / BATCH) * grad
    return current, residual
```

```python
import jax
import jax.numpy as jnp
from jax import lax
from jax.sharding import PartitionSpec as P

HIGH = lax.Precision.HIGHEST


def dot(a, b, contract):
    return lax.dot_general(
        a, b, (contract, ((), ())), precision=HIGH, preferred_element_type=jnp.float32
    )


def swap_cores(x):
    return lax.ppermute(x, "row", [(0, 1), (1, 0)])


def exchange(x):
    return lax.all_to_all(x, "center", 0, 0, tiled=True)


def per_device(dataset, centers, weights, batch_index, targets, gamma):
    shards = lax.axis_size("center")
    cores = lax.axis_size("row")
    assert cores == 2
    me = lax.axis_index("row")
    rows_here = batch_index.shape[1]
    features = dataset.shape[1]
    cols = weights.shape[1]
    count = centers.shape[0]
    batch_total = shards * cores * rows_here
    rate = 0.5 / batch_total

    local = dataset.at[batch_index.reshape(-1)].get(mode="promise_in_bounds")
    rows = exchange(jnp.broadcast_to(local[None], (shards,) + local.shape))
    rows = rows.reshape(-1, features)

    halves = targets.reshape(2, rows_here, 2, cols)
    mine = lax.dynamic_index_in_dim(halves, me, 2, keepdims=False)
    theirs = swap_cores(lax.dynamic_index_in_dim(halves, 1 - me, 2, keepdims=False))
    wanted = jnp.concatenate([mine.reshape(-1, cols), theirs.reshape(-1, cols)], 0)

    center_sq = jnp.sum(centers * centers, axis=1)
    row_sq = jnp.sum(rows * rows, axis=1)
    cross = dot(rows, centers, ((1,), (1,)))
    own = jnp.exp(-gamma[0] * (row_sq[:, None] + center_sq[None, :] - 2.0 * cross))
    other = swap_cores(own)
    split = (shards, 1, 2, rows_here, count)
    kernel = jnp.concatenate([own.reshape(split), other.reshape(split)], 1)
    first = kernel[:, :, 0].reshape(-1, count)
    second = kernel[:, :, 1].reshape(-1, count)
    part = dot(kernel.reshape(-1, count), weights, ((1,), (0,))).reshape(shards, -1, cols)
    gram = dot(second, first, ((1,), (1,)))
    width = -(-batch_total // 128) * 128
    gram = jnp.pad(gram, ((0, 0), (0, width - batch_total))).reshape(shards, -1, width)

    tiles = lambda x: [x[:, :, i : i + 128] for i in range(0, x.shape[2], 128)]
    sent = jnp.concatenate(tiles(part) + tiles(gram), 1)
    got = jnp.sum(exchange(sent), axis=0)
    chip_rows = part.shape[1]
    split_at = chip_rows * (cols // 128)
    done = jnp.concatenate(
        [
            got[i * chip_rows : (i + 1) * chip_rows] - wanted[:, i * 128 : (i + 1) * 128]
            for i in range(cols // 128)
        ]
        + [got[split_at:]],
        0,
    )
    full = exchange(jnp.broadcast_to(done[None], (shards,) + done.shape))
    values = jnp.concatenate(
        [full[:, i * chip_rows : (i + 1) * chip_rows] for i in range(cols // 128)], 2
    )
    gram_rows = gram.shape[1]
    gram = jnp.concatenate(
        [
            full[:, split_at + i * gram_rows : split_at + (i + 1) * gram_rows]
            for i in range(width // 128)
        ],
        2,
    )
    gram = gram.reshape(batch_total, width)[:, :batch_total]
    values = values.reshape(shards, cores, 2, rows_here, cols)
    res0 = values[:, :, 0].reshape(-1, cols)
    res1 = values[:, :, 1].reshape(-1, cols) - rate * dot(gram, res0, ((1,), (0,)))
    grad = dot(first, res0, ((0,), (0,))) + dot(second, res1, ((0,), (0,)))
    new_weights = weights - rate * grad

    chip = lax.dynamic_index_in_dim(
        res1.reshape(shards, cores, rows_here, cols), lax.axis_index("center"), 0, keepdims=False
    )
    back = swap_cores(chip[1])
    residual = jnp.where(
        me == 0,
        jnp.concatenate([chip[0], back], 1),
        jnp.concatenate([back, chip[0]], 1),
    )
    return (new_weights, residual)


def solution(mesh):
    return jax.shard_map(
        per_device,
        mesh=mesh,
        in_specs=(
            P(("groups", "center", "row"), None),
            P(("groups", "center"), None),
            P(("groups", "center"), "row"),
            P(None, ("groups", "center", "row")),
            P(None, ("groups", "center", "row"), None),
            P("groups"),
        ),
        out_specs=(P(("groups", "center"), "row"), P(("groups", "center", "row"), None)),
        check_vma=False,
    )
```

```python
import functools
import math

import jax
import jax.numpy as jnp
from jax import lax
from jax.experimental import pallas as pl
from jax.experimental.pallas import tpu as pltpu
from jax.sharding import PartitionSpec as P

LANES = 128
KEPT_BYTES = 1 << 20


def dot(a, b, contract):
    return lax.dot_general(
        a,
        b,
        (contract, ((), ())),
        precision=lax.Precision.HIGHEST,
        preferred_element_type=jnp.float32,
    )


def small(x):
    return math.prod(x.shape) * 4 <= KEPT_BYTES


def call(body, outs, name, *args):
    args = [a if isinstance(a, tuple) else (a, pltpu.VMEM) for a in args]
    return pl.pallas_call(
        body,
        out_shape=outs,
        in_specs=[pl.BlockSpec(memory_space=space) for _, space in args],
        out_specs=[pl.BlockSpec(memory_space=pltpu.VMEM)] * len(outs),
        name=name,
    )(
        *[
            pltpu.with_memory_space_constraint(a, space)
            if space == pltpu.VMEM and small(a)
            else a
            for a, space in args
        ]
    )


def stored(*shape):
    return jax.ShapeDtypeStruct(shape, jnp.float32)


def kept(*shape):
    return pltpu.VMEM(shape, jnp.float32) if small(stored(*shape)) else stored(*shape)


def swap_cores(x):
    return lax.ppermute(x, "row", [(0, 1), (1, 0)])


def exchange(x):
    return lax.all_to_all(x, "center", 0, 0, tiled=True)


def pick_body(index, gamma, dataset, out, spread):
    spread[...] = jnp.full(spread.shape, gamma[0])
    batches, count = index.shape
    rows = jnp.concatenate(
        [dataset[pl.ds(index[b, j], 1), :] for b in range(batches) for j in range(count)], 0
    )
    out[...] = jnp.broadcast_to(rows[None], out.shape)


def kernel_body(gamma, rows, centers, targets, out):
    x, c = rows[...], centers[...]
    count = c.shape[0]
    row_sq = jnp.sum(x * x, axis=1, keepdims=True)
    center_sq = jnp.sum(c * c, axis=1, keepdims=True)
    center_sq = jnp.broadcast_to(center_sq, (count, LANES)).T[:1]
    cross = dot(x, c, ((1,), (1,)))
    n = x.shape[0]
    out[:n] = jnp.exp(-gamma[:1] * (row_sq + center_sq - 2.0 * cross))
    wanted = target_rows(targets, 1 - lax.axis_index("row"))
    for i, tile in enumerate(wanted):
        out[n + i * tile.shape[0] : n + (i + 1) * tile.shape[0]] = tile


def target_rows(targets, side):
    cols = targets.shape[2] // 2
    both = jnp.concatenate([targets[b] for b in range(targets.shape[0])], 0)
    half = jnp.where(side == 0, both[:, :cols], both[:, cols:])
    return [half[:, i : i + LANES] for i in range(0, cols, LANES)]


def merge_batch(own, other):
    half = own.shape[1] // 2
    low = lax.broadcasted_iota(jnp.int32, own.shape, 1) < half
    return jnp.where(low, pltpu.roll(own, half, 1), other)


def predict_body(each, made, swapped, weights, out):
    shards, _, lanes = out.shape
    n, count = shards * each, made.shape[1]
    w = weights[...]
    a, b = made[:n], swapped[:n]
    tile = 0
    for half in (a, b):
        part = dot(half, w, ((1,), (0,)))
        for i in range(0, w.shape[1], lanes):
            out[:, tile : tile + each] = part[:, i : i + lanes].reshape(shards, each, lanes)
            tile += each
    second = merge_batch(a.reshape(shards, each, count), b.reshape(shards, each, count))
    second = second.reshape(n, count)
    gram = jnp.concatenate([dot(second, a, ((1,), (1,))), dot(second, b, ((1,), (1,)))], 1)
    first = lax.broadcasted_iota(jnp.int32, gram.shape, 1) % each < each // 2
    gram = jnp.where(first, gram, 0.0)
    for i in range(0, gram.shape[1], lanes):
        out[:, tile : tile + each] = gram[:, i : i + lanes].reshape(shards, each, lanes)
        tile += each


def residual_body(got, swapped, targets, out):
    total = jnp.sum(got[...], axis=0)
    mine = target_rows(targets, lax.axis_index("row"))
    each = mine[0].shape[0]
    n = swapped.shape[0] - each * len(mine)
    theirs = [swapped[n + i * each : n + (i + 1) * each] for i in range(len(mine))]
    wanted = mine + theirs
    total = jnp.concatenate(
        [total[i * each : (i + 1) * each] - t for i, t in enumerate(wanted)]
        + [total[each * len(wanted) :]],
        0,
    )
    out[...] = jnp.broadcast_to(total[None], out.shape)


def second_body(rate, full, own_out, other_out, mine_out, theirs_out):
    shards, _, lanes = full.shape
    n, cols = own_out.shape
    each = n // shards
    tiles = cols // lanes
    take = lambda i: full[:, i * each : (i + 1) * each].reshape(n, lanes)
    own = jnp.concatenate([take(i) for i in range(tiles)], 1)
    other = jnp.concatenate([take(i) for i in range(tiles, 2 * tiles)], 1)
    gram = jnp.concatenate([take(i) for i in range(2 * tiles, full.shape[1] // each)], 1)
    step = dot(gram, jnp.concatenate([own, other], 0), ((1,), (0,))) * rate
    step = step.reshape(shards, each, cols)
    half = each // 2
    late = lax.broadcasted_iota(jnp.int32, step.shape, 1) >= half
    move = lambda x: jnp.where(late, x, 0.0).reshape(n, cols)
    own_out[...] = own - move(pltpu.roll(step, half, 1))
    other_out[...] = other - move(step)
    at = lax.axis_index("center") * each
    mine_out[...] = own_out[pl.ds(at, each), :][half:]
    theirs_out[...] = other_out[pl.ds(at, each), :][half:]


def update_body(rate, made, swapped, res_own, res_other, weights, out):
    n = res_own.shape[0]
    k = jnp.concatenate([made[:n], swapped[:n]], 0)
    r = jnp.concatenate([res_own[...], res_other[...]], 0)
    out[...] = weights[...] - rate * dot(k, r, ((0,), (0,)))


def finish_body(mine, back, out):
    first = lax.axis_index("row") == 0
    a, b = mine[...], back[...]
    cols = a.shape[1]
    out[:, :cols] = jnp.where(first, a, b)
    out[:, cols:] = jnp.where(first, b, a)


def per_device(dataset, centers, weights, batch_index, targets, gamma):
    shards = lax.axis_size("center")
    assert lax.axis_size("row") == 2
    batches, rows_here = batch_index.shape
    features = dataset.shape[1]
    count, cols = weights.shape
    each = batches * rows_here
    n = shards * each
    rate = 0.5 / (shards * 2 * rows_here)
    tiles = 2 * (cols // LANES)
    packed = (shards, each * tiles + each * (2 * n // LANES), LANES)

    local, spread = call(
        pick_body,
        [kept(shards, each, features), kept(8, count)],
        "pick",
        (batch_index, pltpu.SMEM),
        (gamma, pltpu.SMEM),
        dataset,
    )
    rows = exchange(local).reshape(n, features)
    (made,) = call(
        kernel_body,
        [kept(n + each * (tiles // 2), count)],
        "kernel",
        spread,
        rows,
        centers,
        targets,
    )
    swapped = swap_cores(made)
    (sent,) = call(functools.partial(predict_body, each), [kept(*packed)], "predict", made, swapped, weights)
    got = exchange(sent)
    (done,) = call(residual_body, [kept(*packed)], "residual", got, swapped, targets)
    full = exchange(done)
    res_own, res_other, mine, theirs = call(
        functools.partial(second_body, rate),
        [kept(n, cols), kept(n, cols), kept(rows_here, cols), kept(rows_here, cols)],
        "second",
        full,
    )
    back = swap_cores(theirs)
    (new_weights,) = call(
        functools.partial(update_body, rate),
        [stored(count, cols)],
        "update",
        made,
        swapped,
        res_own,
        res_other,
        weights,
    )
    (residual,) = call(finish_body, [stored(rows_here, 2 * cols)], "finish", mine, back)
    return (new_weights, residual)


def solution(mesh):
    return jax.shard_map(
        per_device,
        mesh=mesh,
        in_specs=(
            P(("groups", "center", "row"), None),
            P(("groups", "center"), None),
            P(("groups", "center"), "row"),
            P(None, ("groups", "center", "row")),
            P(None, ("groups", "center", "row"), None),
            P("groups"),
        ),
        out_specs=(P(("groups", "center"), "row"), P(("groups", "center", "row"), None)),
        check_vma=False,
    )
```

```python
import functools
import math
from typing import NamedTuple

import jax
import jax.numpy as jnp
from jax import lax
from jax.experimental import pallas as pl
from jax.experimental.pallas import tpu as pltpu
from jax.sharding import PartitionSpec as P

LANES = 128
QUAD = 4
KEPT_BYTES = 1 << 20


class Plan(NamedTuple):
    high: int
    each: int
    col_tiles: int
    width: int
    pack: int

    @property
    def sums(self):
        return 2 * self.col_tiles * self.high

    @property
    def gram_rows(self):
        return self.high // self.pack

    @property
    def gram_tiles(self):
        return self.width * self.pack // LANES

    @property
    def tiles(self):
        return self.sums + self.gram_rows * self.gram_tiles


def dot(a, b, contract):
    return lax.dot_general(
        a,
        b,
        (contract, ((), ())),
        precision=lax.Precision.HIGHEST,
        preferred_element_type=jnp.float32,
    )


def small(x):
    return math.prod(x.shape) * 4 <= KEPT_BYTES


def call(body, outs, name, *args, **kwargs):
    args = [a if isinstance(a, tuple) else (a, pltpu.VMEM) for a in args]
    return pl.pallas_call(
        body,
        out_shape=outs,
        in_specs=[pl.BlockSpec(memory_space=space) for _, space in args],
        out_specs=[pl.BlockSpec(memory_space=pltpu.VMEM)] * len(outs),
        name=name,
        **kwargs,
    )(
        *[
            pltpu.with_memory_space_constraint(a, space)
            if space == pltpu.VMEM and small(a)
            else a
            for a, space in args
        ]
    )


def stored(*shape):
    return jax.ShapeDtypeStruct(shape, jnp.float32)


def kept(*shape):
    return pltpu.VMEM(shape, jnp.float32) if small(stored(*shape)) else stored(*shape)


def swap_cores(x):
    return lax.ppermute(x, "row", [(0, 1), (1, 0)])


def partner(x, bits):
    return lax.ppermute(x, "center", [(i, i ^ bits) for i in range(lax.axis_size("center"))])


def xor_lanes(tiles, stride):
    if stride >= LANES:
        return [tiles[i ^ (stride // LANES)] for i in range(len(tiles))]
    lane = lax.broadcasted_iota(jnp.int32, tiles[0].shape, tiles[0].ndim - 1)
    axis = tiles[0].ndim - 1
    return [
        jnp.where(
            lane & stride != 0, pltpu.roll(t, stride, axis), pltpu.roll(t, LANES - stride, axis)
        )
        for t in tiles
    ]


def seen_by(plan, tiles, q):
    for bit in (1, 2):
        if q & bit:
            tiles = xor_lanes(tiles, bit * plan.high * plan.each)
    return tiles


def pick_body(index, gamma, dataset, out, spread, index_s, gamma_s, data, sems):
    copies = [
        pltpu.make_async_copy(a, b, sems.at[i])
        for i, (a, b) in enumerate(((index, index_s), (gamma, gamma_s), (dataset, data)))
    ]
    for c in copies:
        c.start()
    for c in copies:
        c.wait()
    spread[...] = jnp.full(spread.shape, gamma_s[0])
    batches, count = index.shape
    for b in range(batches):
        for j in range(count):
            at = b * count + j
            out[at : at + 1] = data[pl.ds(index_s[b, j], 1), :]


def center_body(centers, out):
    c = centers[...]
    count = c.shape[0]
    sq = jnp.sum(c * c, axis=1, keepdims=True)
    out[...] = jnp.broadcast_to(sq, (count, LANES)).T[: out.shape[0]]


def kernel_body(gamma, rows, centers, center_sq, out):
    x = rows[...]
    row_sq = jnp.sum(x * x, axis=1, keepdims=True)
    cross = dot(x, centers[...], ((1,), (1,)))
    out[...] = jnp.exp(-gamma[:1] * (row_sq + center_sq[:1] - 2.0 * cross))


def target_rows(targets, side):
    cols = targets.shape[2] // 2
    both = jnp.concatenate([targets[b] for b in range(targets.shape[0])], 0)
    half = jnp.where(side == 0, both[:, :cols], both[:, cols:])
    return [half[:, i : i + LANES] for i in range(0, cols, LANES)]


def target_body(targets, out):
    for i, tile in enumerate(target_rows(targets, 1 - lax.axis_index("row"))):
        out[i * tile.shape[0] : (i + 1) * tile.shape[0]] = tile


def by_batch(own, other):
    axis = own.ndim - 2
    half = own.shape[axis] // 2
    low = lax.broadcasted_iota(jnp.int32, own.shape, axis) < half
    return (
        jnp.where(low, own, pltpu.roll(other, half, axis)),
        jnp.where(low, pltpu.roll(own, half, axis), other),
    )


def predict_body(plan, own, swapped, weights, wanted, targets, k0_out, k1_out, *outs):
    each, high = plan.each, plan.high
    n, count = own.shape
    tiled = lambda x: x.reshape(n // each, each, count)
    k0, k1 = (k.reshape(n, count) for k in by_batch(tiled(own[...]), tiled(swapped[...])))
    k0_out[...] = k0
    k1_out[...] = k1
    w = weights[...]
    span = high * each
    for b, k in enumerate((k0, k1)):
        part = dot(k, w, ((1,), (0,)))
        for q, out in enumerate(outs):
            for c in range(plan.col_tiles):
                tile = part[q * span : (q + 1) * span, c * LANES : (c + 1) * LANES]
                at = (b * plan.col_tiles + c) * high
                out[at : at + high] = tile.reshape(high, each, LANES)
    for c, mine in enumerate(target_rows(targets, lax.axis_index("row"))):
        for b, tile in enumerate(by_batch(mine, wanted[c * each : (c + 1) * each])):
            at = (b * plan.col_tiles + c) * high
            outs[0][at] = outs[0][at] - tile
    gram = dot(k1, jnp.concatenate([k0] * plan.pack, 0), ((1,), (1,)))
    for q, out in enumerate(outs):
        rows = gram[q * span : (q + 1) * span]
        rows = rows.reshape(plan.gram_rows, plan.pack, each, rows.shape[1])
        lane = lax.broadcasted_iota(jnp.int32, rows.shape[:1] + rows.shape[2:], 2)
        packed = rows[:, 0]
        for i in range(1, plan.pack):
            packed = jnp.where(lane >= i * plan.width, rows[:, i], packed)
        tiles = [packed[:, :, i : i + LANES] for i in range(0, packed.shape[2], LANES)]
        for u, tile in enumerate(seen_by(plan, tiles, q)):
            at = plan.sums + u * plan.gram_rows
            out[at : at + plan.gram_rows] = tile


def quad_body(own, *refs):
    *others, out = refs
    total = own[...]
    for other in others:
        total = total + other[...]
    out[...] = total


def high_body(plan, bit, mine, other, out):
    for at in range(0, plan.sums, plan.high):
        for h in range(plan.high):
            out[at + h] = mine[at + h] + other[at + (h ^ bit)]
    t = plan.gram_rows
    step = bit // plan.pack
    for r in range(t):
        tiles = [other[plan.sums + u * t + (r ^ step)] for u in range(plan.gram_tiles)]
        if bit < plan.pack:
            tiles = xor_lanes(tiles, bit * plan.width)
        for u, tile in enumerate(xor_lanes(tiles, bit * plan.each)):
            out[plan.sums + u * t + r] = mine[plan.sums + u * t + r] + tile


def second_body(plan, rate, *refs):
    *packets, out0, out1, mine_out, theirs_out = refs
    span = plan.high * plan.each
    half = plan.each // 2
    for b, out in enumerate((out0, out1)):
        for q, packet in enumerate(packets):
            for c in range(plan.col_tiles):
                at = (b * plan.col_tiles + c) * plan.high
                out[q * span : (q + 1) * span, c * LANES : (c + 1) * LANES] = packet[
                    at : at + plan.high
                ].reshape(span, LANES)
    res0 = out0[...]
    res0 = jnp.concatenate([res0] * plan.pack, 0)
    t = plan.gram_rows
    grams = []
    for q, packet in enumerate(packets):
        tiles = [
            packet[plan.sums + u * t : plan.sums + (u + 1) * t] for u in range(plan.gram_tiles)
        ]
        tiles = seen_by(plan, tiles, q)
        packed = jnp.concatenate(tiles, 2)
        lane = lax.broadcasted_iota(jnp.int32, packed.shape, 2) // plan.width
        rows = [jnp.where(lane == i, packed, 0.0) for i in range(plan.pack)]
        grams.append(jnp.stack(rows, 1).reshape(span, packed.shape[2]))
    gram = jnp.concatenate(grams, 0)
    out1[...] = out1[...] - rate * dot(gram, res0, ((1,), (0,)))
    mine_out[...] = out1[:half]
    theirs_out[...] = out1[half : 2 * half]


def update_body(rate, k0, k1, res0, res1, weights, out):
    grad = dot(k0[...], res0[...], ((0,), (0,))) + dot(k1[...], res1[...], ((0,), (0,)))
    out[...] = weights[...] - rate * grad


def finish_body(mine, back, out):
    first = lax.axis_index("row") == 0
    a, b = mine[...], back[...]
    cols = a.shape[1]
    out[:, :cols] = jnp.where(first, a, b)
    out[:, cols:] = jnp.where(first, b, a)


def per_device(dataset, centers, weights, batch_index, targets, gamma):
    shards = lax.axis_size("center")
    cores = lax.axis_size("row")
    batches, rows_here = batch_index.shape
    assert cores == 2 and batches == 2 and shards % QUAD == 0 and shards & (shards - 1) == 0
    features = dataset.shape[1]
    count, cols = weights.shape
    each = batches * rows_here
    high = shards // QUAD
    span = high * each
    n = shards * each
    width = shards * cores * rows_here
    rate = 0.5 / width
    plan = Plan(high, each, cols // LANES, width, max(1, LANES // width))
    quad = range(1, QUAD)
    bits = [1 << i for i in range(high.bit_length() - 1)]

    local, spread = call(
        pick_body,
        [kept(each, features), kept(8, count)],
        "pick",
        (batch_index, pl.ANY),
        (gamma, pl.ANY),
        (dataset, pl.ANY),
        scratch_shapes=[
            pltpu.SMEM(batch_index.shape, jnp.int32),
            pltpu.SMEM(gamma.shape, jnp.float32),
            pltpu.VMEM(dataset.shape, jnp.float32),
            pltpu.SemaphoreType.DMA((3,)),
        ],
    )
    rows = local
    for bit in bits:
        rows = jnp.concatenate([rows, partner(rows, QUAD * bit)], 0)
    blocks = [rows] + [partner(rows, q) for q in quad]

    (center_sq,) = call(center_body, [kept(8, count)], "center_sq", centers)
    (half,) = call(target_body, [kept(each * plan.col_tiles, LANES)], "targets", targets)
    wanted = swap_cores(half)
    own = [
        call(kernel_body, [kept(span, count)], "kernel", spread, x, centers, center_sq)[0]
        for x in blocks
    ]
    own = jnp.concatenate(own, 0)
    swapped = swap_cores(own)
    packet = (plan.tiles, each, LANES)
    k0, k1, keep, *sent = call(
        functools.partial(predict_body, plan),
        [kept(n, count)] * 2 + [kept(*packet)] * QUAD,
        "predict",
        own,
        swapped,
        weights,
        wanted,
        targets,
    )
    (total,) = call(
        quad_body, [kept(*packet)], "quad", keep, *[partner(s, q) for q, s in zip(quad, sent)]
    )
    for bit in bits:
        (total,) = call(
            functools.partial(high_body, plan, bit),
            [kept(*packet)],
            "high",
            total,
            partner(total, QUAD * bit),
        )
    res0, res1, mine, theirs = call(
        functools.partial(second_body, plan, rate),
        [kept(n, cols)] * 2 + [kept(rows_here, cols)] * 2,
        "second",
        total,
        *[partner(total, q) for q in quad],
    )
    back = swap_cores(theirs)
    (new_weights,) = call(
        functools.partial(update_body, rate),
        [stored(count, cols)],
        "update",
        k0,
        k1,
        res0,
        res1,
        weights,
    )
    (residual,) = call(finish_body, [stored(rows_here, 2 * cols)], "finish", mine, back)
    return (new_weights, residual)


def solution(mesh):
    return jax.shard_map(
        per_device,
        mesh=mesh,
        in_specs=(
            P(("groups", "center", "row"), None),
            P(("groups", "center"), None),
            P(("groups", "center"), "row"),
            P(None, ("groups", "center", "row")),
            P(None, ("groups", "center", "row"), None),
            P("groups"),
        ),
        out_specs=(P(("groups", "center"), "row"), P(("groups", "center", "row"), None)),
        check_vma=False,
    )
```

```python
import functools
import math
from typing import NamedTuple

import jax
import jax.numpy as jnp
from jax import lax
from jax.experimental import pallas as pl
from jax.experimental.pallas import tpu as pltpu
from jax.sharding import PartitionSpec as P

LANES = 128
QUAD = 4
KEPT_BYTES = 1 << 20


class Plan(NamedTuple):
    high: int
    each: int
    col_tiles: int
    width: int
    pack: int

    @property
    def sums(self):
        return 2 * self.col_tiles * self.high

    @property
    def gram_rows(self):
        return self.high // self.pack

    @property
    def gram_tiles(self):
        return self.width * self.pack // LANES

    @property
    def tiles(self):
        return self.sums + self.gram_rows * self.gram_tiles


def dot(a, b, contract):
    return lax.dot_general(
        a,
        b,
        (contract, ((), ())),
        precision=lax.Precision.HIGHEST,
        preferred_element_type=jnp.float32,
    )


def small(x):
    return math.prod(x.shape) * 4 <= KEPT_BYTES


def call(body, outs, name, *args, **kwargs):
    args = [a if isinstance(a, tuple) else (a, pltpu.VMEM) for a in args]
    return pl.pallas_call(
        body,
        out_shape=outs,
        in_specs=[pl.BlockSpec(memory_space=space) for _, space in args],
        out_specs=[pl.BlockSpec(memory_space=pltpu.VMEM)] * len(outs),
        name=name,
        **kwargs,
    )(
        *[
            pltpu.with_memory_space_constraint(a, space)
            if space == pltpu.VMEM and small(a)
            else a
            for a, space in args
        ]
    )


def stored(*shape):
    return jax.ShapeDtypeStruct(shape, jnp.float32)


def kept(*shape):
    return pltpu.VMEM(shape, jnp.float32) if small(stored(*shape)) else stored(*shape)


def swap_cores(x):
    return lax.ppermute(x, "row", [(0, 1), (1, 0)])


def partner(x, bits):
    return lax.ppermute(x, "center", [(i, i ^ bits) for i in range(lax.axis_size("center"))])


def across(x, bits):
    pairs = [
        (2 * i + core, 2 * (i ^ bits) + 1 - core)
        for i in range(lax.axis_size("center"))
        for core in range(2)
    ]
    return lax.ppermute(x, ("center", "row"), pairs)


def xor_lanes(tiles, stride):
    if stride >= LANES:
        return [tiles[i ^ (stride // LANES)] for i in range(len(tiles))]
    lane = lax.broadcasted_iota(jnp.int32, tiles[0].shape, tiles[0].ndim - 1)
    axis = tiles[0].ndim - 1
    return [
        jnp.where(
            lane & stride != 0, pltpu.roll(t, stride, axis), pltpu.roll(t, LANES - stride, axis)
        )
        for t in tiles
    ]


def seen_by(plan, tiles, q):
    for bit in (1, 2):
        if q & bit:
            tiles = xor_lanes(tiles, bit * plan.high * plan.each)
    return tiles


def pick_body(index, dataset, out, index_s, data, sems):
    copies = [
        pltpu.make_async_copy(a, b, sems.at[i])
        for i, (a, b) in enumerate(((index, index_s), (dataset, data)))
    ]
    for c in copies:
        c.start()
    for c in copies:
        c.wait()
    batches, count = index.shape
    for b in range(batches):
        for j in range(count):
            at = b * count + j
            out[at : at + 1] = data[pl.ds(index_s[b, j], 1), :]


def prepare_body(centers, centers_out, sq_out, sem):
    copy = pltpu.make_async_copy(centers, centers_out, sem)
    copy.start()
    copy.wait()
    c = centers_out[...]
    sq = jnp.sum(c * c, axis=1, keepdims=True)
    sq_out[...] = jnp.broadcast_to(sq, (c.shape[0], LANES)).T[: sq_out.shape[0]]


def kernel_body(gamma, rows, centers, center_sq, out):
    x = rows[...]
    row_sq = jnp.sum(x * x, axis=1, keepdims=True)
    cross = dot(x, centers[...], ((1,), (1,)))
    out[...] = jnp.exp(-gamma[:1] * (row_sq + center_sq[:1] - 2.0 * cross))


def by_batch(is_first, mine, theirs):
    first, second = jnp.where(is_first, mine, theirs), jnp.where(is_first, theirs, mine)
    half = mine.shape[0] // 2
    low = lax.broadcasted_iota(jnp.int32, mine.shape, 0) < half
    return (
        jnp.where(low, first, pltpu.roll(second, half, 0)),
        jnp.where(low, pltpu.roll(first, half, 0), second),
    )


def target_tiles(targets, side):
    cols = targets.shape[2] // 2
    both = jnp.concatenate([targets[b] for b in range(targets.shape[0])], 0)
    half = jnp.where(side == 0, both[:, :cols], both[:, cols:])
    return [half[:, i : i + LANES] for i in range(0, cols, LANES)]


def predict_body(plan, *refs):
    own, swapped, w_mine, w_theirs, t_mine, t_theirs, k0_out, k1_out, *outs = refs
    each, high = plan.each, plan.high
    n = own.shape[0]
    me = lax.axis_index("row")
    span = high * each
    for q in range(QUAD):
        for h in range(high):
            at = q * span + h * each
            crossed = (q > 0) ^ (h.bit_count() & 1)
            tile = slice(at, at + each)
            k0_out[tile], k1_out[tile] = by_batch(me == crossed, own[tile], swapped[tile])
    k0, k1 = k0_out[...], k1_out[...]
    for b, k in enumerate((k0, k1)):
        kept_part = dot(k[:span], w_theirs[...], ((1,), (0,)))
        sent_part = dot(k[span:], w_mine[...], ((1,), (0,)))
        part = jnp.concatenate([kept_part, sent_part], 0)
        for q, out in enumerate(outs):
            for c in range(plan.col_tiles):
                tile = part[q * span : (q + 1) * span, c * LANES : (c + 1) * LANES]
                at = (b * plan.col_tiles + c) * high
                out[at : at + high] = tile.reshape(high, each, LANES)
    for c, (mine, theirs) in enumerate(
        zip(target_tiles(t_mine, 1 - me), target_tiles(t_theirs, 1 - me))
    ):
        for b, tile in enumerate(by_batch(me == 0, mine, theirs)):
            at = (b * plan.col_tiles + c) * high
            outs[0][at] = outs[0][at] - tile
    gram = dot(k1, jnp.concatenate([k0] * plan.pack, 0), ((1,), (1,)))
    for q, out in enumerate(outs):
        rows = gram[q * span : (q + 1) * span]
        rows = rows.reshape(plan.gram_rows, plan.pack, each, rows.shape[1])
        lane = lax.broadcasted_iota(jnp.int32, rows.shape[:1] + rows.shape[2:], 2)
        packed = rows[:, 0]
        for i in range(1, plan.pack):
            packed = jnp.where(lane >= i * plan.width, rows[:, i], packed)
        tiles = [packed[:, :, i : i + LANES] for i in range(0, packed.shape[2], LANES)]
        for u, tile in enumerate(seen_by(plan, tiles, q)):
            at = plan.sums + u * plan.gram_rows
            out[at : at + plan.gram_rows] = tile


def quad_body(own, *refs):
    *others, out = refs
    total = own[...]
    for other in others:
        total = total + other[...]
    out[...] = total


def high_body(plan, bit, mine, other, out):
    for at in range(0, plan.sums, plan.high):
        for h in range(plan.high):
            out[at + h] = mine[at + h] + other[at + (h ^ bit)]
    t = plan.gram_rows
    step = bit // plan.pack
    for r in range(t):
        tiles = [other[plan.sums + u * t + (r ^ step)] for u in range(plan.gram_tiles)]
        if bit < plan.pack:
            tiles = xor_lanes(tiles, bit * plan.width)
        for u, tile in enumerate(xor_lanes(tiles, bit * plan.each)):
            out[plan.sums + u * t + r] = mine[plan.sums + u * t + r] + tile


def second_body(plan, rate, *refs):
    *packets, out0, out1, mine_out, theirs_out = refs
    span = plan.high * plan.each
    half = plan.each // 2
    for b, out in enumerate((out0, out1)):
        for q, packet in enumerate(packets):
            for c in range(plan.col_tiles):
                at = (b * plan.col_tiles + c) * plan.high
                out[q * span : (q + 1) * span, c * LANES : (c + 1) * LANES] = packet[
                    at : at + plan.high
                ].reshape(span, LANES)
    res0 = out0[...]
    res0 = jnp.concatenate([res0] * plan.pack, 0)
    t = plan.gram_rows
    grams = []
    for q, packet in enumerate(packets):
        tiles = [
            packet[plan.sums + u * t : plan.sums + (u + 1) * t] for u in range(plan.gram_tiles)
        ]
        tiles = seen_by(plan, tiles, q)
        packed = jnp.concatenate(tiles, 2)
        lane = lax.broadcasted_iota(jnp.int32, packed.shape, 2) // plan.width
        rows = [jnp.where(lane == i, packed, 0.0) for i in range(plan.pack)]
        grams.append(jnp.stack(rows, 1).reshape(span, packed.shape[2]))
    gram = jnp.concatenate(grams, 0)
    out1[...] = out1[...] - rate * dot(gram, res0, ((1,), (0,)))
    first = lax.axis_index("row") == 0
    a, b = out1[:half], out1[half : 2 * half]
    mine_out[...] = jnp.where(first, a, b)
    theirs_out[...] = jnp.where(first, b, a)


def update_body(rate, k0, k1, res0, res1, weights, out):
    grad = dot(k0[...], res0[...], ((0,), (0,))) + dot(k1[...], res1[...], ((0,), (0,)))
    out[...] = weights[...] - rate * grad


def finish_body(mine, back, out):
    first = lax.axis_index("row") == 0
    a, b = mine[...], back[...]
    cols = a.shape[1]
    out[:, :cols] = jnp.where(first, a, b)
    out[:, cols:] = jnp.where(first, b, a)


def per_device(dataset, centers, weights, batch_index, targets, gamma):
    shards = lax.axis_size("center")
    cores = lax.axis_size("row")
    batches, rows_here = batch_index.shape
    assert cores == 2 and batches == 2 and shards % QUAD == 0 and shards & (shards - 1) == 0
    features = dataset.shape[1]
    count, cols = weights.shape
    each = batches * rows_here
    high = shards // QUAD
    span = high * each
    n = shards * each
    width = shards * cores * rows_here
    rate = 0.5 / width
    plan = Plan(high, each, cols // LANES, width, max(1, LANES // width))
    quad = range(1, QUAD)
    bits = [1 << i for i in range(high.bit_length() - 1)]

    (local,) = call(
        pick_body,
        [kept(each, features)],
        "pick",
        (batch_index, pl.ANY),
        (dataset, pl.ANY),
        scratch_shapes=[
            pltpu.SMEM(batch_index.shape, jnp.int32),
            pltpu.VMEM(dataset.shape, jnp.float32),
            pltpu.SemaphoreType.DMA((2,)),
        ],
    )
    held, center_sq = call(
        prepare_body,
        [kept(count, features), kept(8, count)],
        "prepare",
        (centers, pl.ANY),
        scratch_shapes=[pltpu.SemaphoreType.DMA],
    )
    spread = jnp.broadcast_to(gamma, (8, count))
    rows = local
    for bit in bits:
        rows = jnp.concatenate([rows, across(rows, QUAD * bit)], 0)
    rows, held, center_sq, spread = lax.optimization_barrier((rows, held, center_sq, spread))
    own = [
        call(kernel_body, [kept(span, count)], "kernel", spread, x, held, center_sq)[0]
        for x in [rows] + [across(rows, q) for q in quad]
    ]
    own = jnp.concatenate(own, 0)
    packet = (plan.tiles, each, LANES)
    k0, k1, keep, *sent = call(
        functools.partial(predict_body, plan),
        [kept(n, count)] * 2 + [kept(*packet)] * QUAD,
        "predict",
        own,
        swap_cores(own),
        weights,
        swap_cores(weights),
        targets,
        swap_cores(targets),
    )
    (total,) = call(
        quad_body, [kept(*packet)], "quad", keep, *[across(s, q) for q, s in zip(quad, sent)]
    )
    for bit in bits:
        (total,) = call(
            functools.partial(high_body, plan, bit),
            [kept(*packet)],
            "high",
            total,
            partner(total, QUAD * bit),
        )
    res0, res1, mine, theirs = call(
        functools.partial(second_body, plan, rate),
        [kept(n, cols)] * 2 + [kept(rows_here, cols)] * 2,
        "second",
        swap_cores(total),
        *[across(total, q) for q in quad],
    )
    back = swap_cores(theirs)
    (new_weights,) = call(
        functools.partial(update_body, rate),
        [stored(count, cols)],
        "update",
        k0,
        k1,
        res0,
        res1,
        weights,
    )
    (residual,) = call(finish_body, [stored(rows_here, 2 * cols)], "finish", mine, back)
    return (new_weights, residual)


def solution(mesh):
    return jax.shard_map(
        per_device,
        mesh=mesh,
        in_specs=(
            P(("groups", "center", "row"), None),
            P(("groups", "center"), None),
            P(("groups", "center"), "row"),
            P(None, ("groups", "center", "row")),
            P(None, ("groups", "center", "row"), None),
            P("groups"),
        ),
        out_specs=(P(("groups", "center"), "row"), P(("groups", "center", "row"), None)),
        check_vma=False,
    )
```

```python
import functools
import math
from typing import NamedTuple

import jax
import jax.numpy as jnp
from jax import lax
from jax.experimental import pallas as pl
from jax.experimental.pallas import tpu as pltpu
from jax.sharding import PartitionSpec as P

LANES = 128
QUAD = 4
KEPT_BYTES = 1 << 20


class Plan(NamedTuple):
    high: int
    each: int
    col_tiles: int
    width: int
    pack: int

    @property
    def sums(self):
        return 2 * self.col_tiles * self.high

    @property
    def gram_rows(self):
        return self.high // self.pack

    @property
    def gram_tiles(self):
        return self.width * self.pack // LANES

    @property
    def tiles(self):
        return self.sums + self.gram_rows * self.gram_tiles


def dot(a, b, contract):
    return lax.dot_general(
        a,
        b,
        (contract, ((), ())),
        precision=lax.Precision.HIGHEST,
        preferred_element_type=jnp.float32,
    )


def small(x):
    return math.prod(x.shape) * jnp.dtype(x.dtype).itemsize <= KEPT_BYTES


def call(body, outs, name, *args, **kwargs):
    args = [a if isinstance(a, tuple) else (a, pltpu.VMEM) for a in args]
    return pl.pallas_call(
        body,
        out_shape=outs,
        in_specs=[pl.BlockSpec(memory_space=space) for _, space in args],
        out_specs=[pl.BlockSpec(memory_space=pltpu.VMEM)] * len(outs),
        name=name,
        **kwargs,
    )(
        *[
            pltpu.with_memory_space_constraint(a, space)
            if space == pltpu.VMEM and small(a)
            else a
            for a, space in args
        ]
    )


def stored(*shape):
    return jax.ShapeDtypeStruct(shape, jnp.float32)


def kept(*shape):
    return pltpu.VMEM(shape, jnp.float32) if small(stored(*shape)) else stored(*shape)


def swap_cores(x):
    return lax.ppermute(x, "row", [(0, 1), (1, 0)])


def partner(x, bits):
    return lax.ppermute(x, "center", [(i, i ^ bits) for i in range(lax.axis_size("center"))])


def across(x, bits):
    pairs = [
        (2 * i + core, 2 * (i ^ bits) + 1 - core)
        for i in range(lax.axis_size("center"))
        for core in range(2)
    ]
    return lax.ppermute(x, ("center", "row"), pairs)


def xor_lanes(tiles, stride):
    if stride >= LANES:
        return [tiles[i ^ (stride // LANES)] for i in range(len(tiles))]
    lane = lax.broadcasted_iota(jnp.int32, tiles[0].shape, tiles[0].ndim - 1)
    axis = tiles[0].ndim - 1
    return [
        jnp.where(
            lane & stride != 0, pltpu.roll(t, stride, axis), pltpu.roll(t, LANES - stride, axis)
        )
        for t in tiles
    ]


def seen_by(plan, tiles, q):
    for bit in (1, 2):
        if q & bit:
            tiles = xor_lanes(tiles, bit * plan.high * plan.each)
    return tiles


def pick_body(index, dataset, out, index_s, data, sems):
    copies = [
        pltpu.make_async_copy(a, b, sems.at[i])
        for i, (a, b) in enumerate(((index, index_s), (dataset, data)))
    ]
    for c in copies:
        c.start()
    for c in copies:
        c.wait()
    batches, count = index.shape
    for b in range(batches):
        for j in range(count):
            at = b * count + j
            out[at : at + 1] = data[pl.ds(index_s[b, j], 1), :]


def parts(x):
    out = []
    for _ in range(3):
        out.append(x.astype(jnp.bfloat16))
        x = x - out[-1].astype(jnp.float32)
    return out


def prepare_body(centers, targets, split_out, row_out, targets_out, held, sems):
    copies = [
        pltpu.make_async_copy(a, b, sems.at[i])
        for i, (a, b) in enumerate(((centers, held), (targets, targets_out)))
    ]
    for c in copies:
        c.start()
    for c in copies:
        c.wait()
    c = held[...]
    for i, part in enumerate(parts(c)):
        split_out[i] = part
    sq = jnp.sum(c * c, axis=1, keepdims=True)
    row_out[...] = jnp.broadcast_to(sq, (c.shape[0], LANES)).T[: row_out.shape[0]]


def kernel_body(gamma, rows, split, row, out):
    x = rows[...]
    n = x.shape[0]
    row_sq = jnp.sum(x * x, axis=1, keepdims=True)
    xs = parts(x)
    cross = 0.0
    for i in (2, 1, 0):
        left = jnp.concatenate(xs[: 3 - i], 0)
        part = lax.dot_general(
            left, split[i], (((1,), (1,)), ((), ())), preferred_element_type=jnp.float32
        )
        for j in reversed(range(3 - i)):
            cross = cross + part[j * n : (j + 1) * n]
    out[...] = jnp.exp(-gamma[:1] * (row_sq + row[:1] - 2.0 * cross))


def by_batch(is_first, mine, theirs):
    first, second = jnp.where(is_first, mine, theirs), jnp.where(is_first, theirs, mine)
    half = mine.shape[0] // 2
    low = lax.broadcasted_iota(jnp.int32, mine.shape, 0) < half
    return (
        jnp.where(low, first, pltpu.roll(second, half, 0)),
        jnp.where(low, pltpu.roll(first, half, 0), second),
    )


def target_tiles(targets, side):
    cols = targets.shape[2] // 2
    both = jnp.concatenate([targets[b] for b in range(targets.shape[0])], 0)
    half = jnp.where(side == 0, both[:, :cols], both[:, cols:])
    return [half[:, i : i + LANES] for i in range(0, cols, LANES)]


def predict_body(plan, *refs):
    own, swapped, w_mine, w_theirs, t_mine, t_theirs, k0_out, k1_out, *outs = refs
    each, high = plan.each, plan.high
    n = own.shape[0]
    me = lax.axis_index("row")
    span = high * each
    for q in range(QUAD):
        for h in range(high):
            at = q * span + h * each
            crossed = (q > 0) ^ (h.bit_count() & 1)
            tile = slice(at, at + each)
            k0_out[tile], k1_out[tile] = by_batch(me == crossed, own[tile], swapped[tile])
    k0, k1 = k0_out[...], k1_out[...]
    for b, k in enumerate((k0, k1)):
        kept_part = dot(k[:span], w_theirs[...], ((1,), (0,)))
        sent_part = dot(k[span:], w_mine[...], ((1,), (0,)))
        part = jnp.concatenate([kept_part, sent_part], 0)
        for q, out in enumerate(outs):
            for c in range(plan.col_tiles):
                tile = part[q * span : (q + 1) * span, c * LANES : (c + 1) * LANES]
                at = (b * plan.col_tiles + c) * high
                out[at : at + high] = tile.reshape(high, each, LANES)
    for c, (mine, theirs) in enumerate(
        zip(target_tiles(t_mine, 1 - me), target_tiles(t_theirs, 1 - me))
    ):
        for b, tile in enumerate(by_batch(me == 0, mine, theirs)):
            at = (b * plan.col_tiles + c) * high
            outs[0][at] = outs[0][at] - tile
    gram = dot(k1, jnp.concatenate([k0] * plan.pack, 0), ((1,), (1,)))
    for q, out in enumerate(outs):
        rows = gram[q * span : (q + 1) * span]
        rows = rows.reshape(plan.gram_rows, plan.pack, each, rows.shape[1])
        lane = lax.broadcasted_iota(jnp.int32, rows.shape[:1] + rows.shape[2:], 2)
        packed = rows[:, 0]
        for i in range(1, plan.pack):
            packed = jnp.where(lane >= i * plan.width, rows[:, i], packed)
        tiles = [packed[:, :, i : i + LANES] for i in range(0, packed.shape[2], LANES)]
        for u, tile in enumerate(seen_by(plan, tiles, q)):
            at = plan.sums + u * plan.gram_rows
            out[at : at + plan.gram_rows] = tile


def quad_body(own, *refs):
    *others, out = refs
    total = own[...]
    for other in others:
        total = total + other[...]
    out[...] = total


def high_body(plan, bit, mine, other, out):
    for at in range(0, plan.sums, plan.high):
        for h in range(plan.high):
            out[at + h] = mine[at + h] + other[at + (h ^ bit)]
    t = plan.gram_rows
    step = bit // plan.pack
    for r in range(t):
        tiles = [other[plan.sums + u * t + (r ^ step)] for u in range(plan.gram_tiles)]
        if bit < plan.pack:
            tiles = xor_lanes(tiles, bit * plan.width)
        for u, tile in enumerate(xor_lanes(tiles, bit * plan.each)):
            out[plan.sums + u * t + r] = mine[plan.sums + u * t + r] + tile


def second_body(plan, rate, *refs):
    *packets, out0, out1, mine_out, theirs_out = refs
    span = plan.high * plan.each
    half = plan.each // 2
    for b, out in enumerate((out0, out1)):
        for q, packet in enumerate(packets):
            for c in range(plan.col_tiles):
                at = (b * plan.col_tiles + c) * plan.high
                out[q * span : (q + 1) * span, c * LANES : (c + 1) * LANES] = packet[
                    at : at + plan.high
                ].reshape(span, LANES)
    res0 = out0[...]
    res0 = jnp.concatenate([res0] * plan.pack, 0)
    t = plan.gram_rows
    grams = []
    for q, packet in enumerate(packets):
        tiles = [
            packet[plan.sums + u * t : plan.sums + (u + 1) * t] for u in range(plan.gram_tiles)
        ]
        tiles = seen_by(plan, tiles, q)
        packed = jnp.concatenate(tiles, 2)
        lane = lax.broadcasted_iota(jnp.int32, packed.shape, 2) // plan.width
        rows = [jnp.where(lane == i, packed, 0.0) for i in range(plan.pack)]
        grams.append(jnp.stack(rows, 1).reshape(span, packed.shape[2]))
    gram = jnp.concatenate(grams, 0)
    out1[...] = out1[...] - rate * dot(gram, res0, ((1,), (0,)))
    first = lax.axis_index("row") == 0
    a, b = out1[:half], out1[half : 2 * half]
    mine_out[...] = jnp.where(first, a, b)
    theirs_out[...] = jnp.where(first, b, a)


def update_body(rate, k0, k1, res0, res1, weights, out):
    grad = dot(k0[...], res0[...], ((0,), (0,))) + dot(k1[...], res1[...], ((0,), (0,)))
    out[...] = weights[...] - rate * grad


def finish_body(mine, back, out):
    first = lax.axis_index("row") == 0
    a, b = mine[...], back[...]
    cols = a.shape[1]
    out[:, :cols] = jnp.where(first, a, b)
    out[:, cols:] = jnp.where(first, b, a)


def per_device(dataset, centers, weights, batch_index, targets, gamma):
    shards = lax.axis_size("center")
    cores = lax.axis_size("row")
    batches, rows_here = batch_index.shape
    assert cores == 2 and batches == 2 and shards % QUAD == 0 and shards & (shards - 1) == 0
    features = dataset.shape[1]
    count, cols = weights.shape
    each = batches * rows_here
    high = shards // QUAD
    span = high * each
    n = shards * each
    width = shards * cores * rows_here
    rate = 0.5 / width
    plan = Plan(high, each, cols // LANES, width, max(1, LANES // width))
    quad = range(1, QUAD)
    bits = [1 << i for i in range(high.bit_length() - 1)]

    (local,) = call(
        pick_body,
        [kept(each, features)],
        "pick",
        (batch_index, pl.ANY),
        (dataset, pl.ANY),
        scratch_shapes=[
            pltpu.SMEM(batch_index.shape, jnp.int32),
            pltpu.VMEM(dataset.shape, jnp.float32),
            pltpu.SemaphoreType.DMA((2,)),
        ],
    )
    split, row, targets = call(
        prepare_body,
        [
            pltpu.VMEM((3, count, features), jnp.bfloat16),
            kept(8, count),
            kept(*targets.shape),
        ],
        "prepare",
        (centers, pl.ANY),
        (targets, pl.ANY),
        scratch_shapes=[
            pltpu.VMEM(centers.shape, jnp.float32),
            pltpu.SemaphoreType.DMA((2,)),
        ],
    )
    spread = jnp.broadcast_to(gamma, (8, count))
    rows = local
    for bit in bits:
        rows = jnp.concatenate([rows, across(rows, QUAD * bit)], 0)
    rows, split, row, targets = lax.optimization_barrier((rows, split, row, targets))
    own = [
        call(kernel_body, [kept(span, count)], "kernel", spread, x, split, row)[0]
        for x in [rows] + [across(rows, q) for q in quad]
    ]
    own[0], weights_other, targets_other = lax.optimization_barrier(
        (own[0], swap_cores(weights), swap_cores(targets))
    )
    own = jnp.concatenate(own, 0)
    packet = (plan.tiles, each, LANES)
    k0, k1, keep, *sent = call(
        functools.partial(predict_body, plan),
        [kept(n, count)] * 2 + [kept(*packet)] * QUAD,
        "predict",
        own,
        swap_cores(own),
        weights,
        weights_other,
        targets,
        targets_other,
    )
    (total,) = call(
        quad_body,
        [kept(*packet)],
        "quad",
        keep,
        *[across(sent[q - 1], q) for q in reversed(quad)],
    )
    for bit in bits:
        (total,) = call(
            functools.partial(high_body, plan, bit),
            [kept(*packet)],
            "high",
            total,
            partner(total, QUAD * bit),
        )
    res0, res1, mine, theirs = call(
        functools.partial(second_body, plan, rate),
        [kept(n, cols)] * 2 + [kept(rows_here, cols)] * 2,
        "second",
        swap_cores(total),
        *[across(total, q) for q in quad],
    )
    back = swap_cores(theirs)
    (new_weights,) = call(
        functools.partial(update_body, rate),
        [stored(count, cols)],
        "update",
        k0,
        k1,
        res0,
        res1,
        weights,
    )
    (residual,) = call(finish_body, [stored(rows_here, 2 * cols)], "finish", mine, back)
    return (new_weights, residual)


def solution(mesh):
    return jax.shard_map(
        per_device,
        mesh=mesh,
        in_specs=(
            P(("groups", "center", "row"), None),
            P(("groups", "center"), None),
            P(("groups", "center"), "row"),
            P(None, ("groups", "center", "row")),
            P(None, ("groups", "center", "row"), None),
            P("groups"),
        ),
        out_specs=(P(("groups", "center"), "row"), P(("groups", "center", "row"), None)),
        check_vma=False,
    )
```

```python
import functools
import math
from typing import NamedTuple

import jax
import jax.numpy as jnp
from jax import lax
from jax.experimental import pallas as pl
from jax.experimental.pallas import tpu as pltpu
from jax.sharding import PartitionSpec as P

LANES = 128
QUAD = 4
KEPT_BYTES = 400 << 10


class Plan(NamedTuple):
    high: int
    each: int
    col_tiles: int
    width: int
    pack: int

    @property
    def sums(self):
        return 2 * self.col_tiles * self.high

    @property
    def gram_rows(self):
        return self.high // self.pack

    @property
    def gram_tiles(self):
        return self.width * self.pack // LANES

    @property
    def tiles(self):
        return self.sums + self.gram_rows * self.gram_tiles


def dot(a, b, contract):
    return lax.dot_general(
        a,
        b,
        (contract, ((), ())),
        precision=lax.Precision.HIGHEST,
        preferred_element_type=jnp.float32,
    )


def small(x):
    bytes_each = jnp.dtype(x.dtype).itemsize
    return bytes_each == 2 or math.prod(x.shape) * bytes_each <= KEPT_BYTES


def call(body, outs, name, *args, out_space=pltpu.VMEM, **kwargs):
    args = [a if isinstance(a, tuple) else (a, pltpu.VMEM) for a in args]
    return pl.pallas_call(
        body,
        out_shape=outs,
        in_specs=[pl.BlockSpec(memory_space=space) for _, space in args],
        out_specs=[pl.BlockSpec(memory_space=out_space)] * len(outs),
        name=name,
        **kwargs,
    )(
        *[
            pltpu.with_memory_space_constraint(a, space)
            if space == pltpu.VMEM and small(a)
            else a
            for a, space in args
        ]
    )


def stored(*shape):
    return jax.ShapeDtypeStruct(shape, jnp.float32)


def kept(*shape):
    return pltpu.VMEM(shape, jnp.float32) if small(stored(*shape)) else stored(*shape)


def swap_cores(x):
    return lax.ppermute(x, "row", [(0, 1), (1, 0)])


def partner(x, bits):
    return lax.ppermute(x, "center", [(i, i ^ bits) for i in range(lax.axis_size("center"))])


def across(x, bits):
    pairs = [
        (2 * i + core, 2 * (i ^ bits) + 1 - core)
        for i in range(lax.axis_size("center"))
        for core in range(2)
    ]
    return lax.ppermute(x, ("center", "row"), pairs)


def xor_lanes(tiles, stride):
    if stride >= LANES:
        return [tiles[i ^ (stride // LANES)] for i in range(len(tiles))]
    lane = lax.broadcasted_iota(jnp.int32, tiles[0].shape, tiles[0].ndim - 1)
    axis = tiles[0].ndim - 1
    return [
        jnp.where(
            lane & stride != 0, pltpu.roll(t, stride, axis), pltpu.roll(t, LANES - stride, axis)
        )
        for t in tiles
    ]


def seen_by(plan, tiles, q):
    for bit in (1, 2):
        if q & bit:
            tiles = xor_lanes(tiles, bit * plan.high * plan.each)
    return tiles


def pick_body(index, dataset, out, index_s, data, sems):
    copies = [
        pltpu.make_async_copy(a, b, sems.at[i])
        for i, (a, b) in enumerate(((index, index_s), (dataset, data)))
    ]
    for c in copies:
        c.start()
    for c in copies:
        c.wait()
    batches, count = index.shape
    for b in range(batches):
        for j in range(count):
            at = b * count + j
            out[at : at + 1] = data[pl.ds(index_s[b, j], 1), :]


def parts(x):
    out = []
    for _ in range(3):
        out.append(x.astype(jnp.bfloat16))
        x = x - out[-1].astype(jnp.float32)
    return out


def parts_dot(left, right, axis):
    n = left[0].shape[0]
    total = 0.0
    for i in (2, 1, 0):
        part = lax.dot_general(
            jnp.concatenate(left[: 3 - i], 0),
            right[i],
            (((1,), (axis,)), ((), ())),
            preferred_element_type=jnp.float32,
        )
        for j in reversed(range(3 - i)):
            total = total + part[j * n : (j + 1) * n]
    return total


def prepare_body(centers, targets, split_out, row_out, targets_out, held, sems):
    copies = [
        pltpu.make_async_copy(a, b, sems.at[i])
        for i, (a, b) in enumerate(((centers, held), (targets, targets_out)))
    ]
    for c in copies:
        c.start()
    for c in copies:
        c.wait()
    c = held[...]
    for i, part in enumerate(parts(c)):
        split_out[i] = part
    sq = jnp.sum(c * c, axis=1, keepdims=True)
    row_out[...] = jnp.broadcast_to(sq, (c.shape[0], LANES)).T[: row_out.shape[0]]


def kernel_body(gamma, rows, split, row, out):
    x = rows[...]
    row_sq = jnp.sum(x * x, axis=1, keepdims=True)
    cross = parts_dot(parts(x), split, 1)
    out[...] = jnp.exp(-gamma[:1] * (row_sq + row[:1] - 2.0 * cross))


def by_batch(is_first, mine, theirs):
    first, second = jnp.where(is_first, mine, theirs), jnp.where(is_first, theirs, mine)
    half = mine.shape[0] // 2
    low = lax.broadcasted_iota(jnp.int32, mine.shape, 0) < half
    return (
        jnp.where(low, first, pltpu.roll(second, half, 0)),
        jnp.where(low, pltpu.roll(first, half, 0), second),
    )


def target_tiles(targets, side):
    cols = targets.shape[2] // 2
    both = jnp.concatenate([targets[b] for b in range(targets.shape[0])], 0)
    half = jnp.where(side == 0, both[:, :cols], both[:, cols:])
    return [half[:, i : i + LANES] for i in range(0, cols, LANES)]


def half_sums(plan, k, split):
    span = plan.high * plan.each
    return jnp.concatenate(
        [
            parts_dot(parts(k[:span]), split[1], 0),
            parts_dot(parts(k[span:]), split[0], 0),
        ],
        0,
    )


def weights_body(plan, own, w_mine, w_theirs, split_out, out):
    for side, w in enumerate((w_mine, w_theirs)):
        for i, part in enumerate(parts(w[...])):
            split_out[side, i] = part
    out[...] = half_sums(plan, own[...], split_out)


def predict_body(plan, *refs):
    own, swapped, mine_sums, split, t_mine, t_theirs, k0_out, k1_out, *outs = refs
    each, high = plan.each, plan.high
    me = lax.axis_index("row")
    span = high * each
    sums = half_sums(plan, swapped[...], split)
    for q in range(QUAD):
        for h in range(high):
            at = q * span + h * each
            crossed = (q > 0) ^ (h.bit_count() & 1)
            tile = slice(at, at + each)
            k0_out[tile], k1_out[tile] = by_batch(me == crossed, own[tile], swapped[tile])
            for b, rows in enumerate(by_batch(me == crossed, mine_sums[tile], sums[tile])):
                for c in range(plan.col_tiles):
                    to = (b * plan.col_tiles + c) * high + h
                    outs[q][to] = rows[:, c * LANES : (c + 1) * LANES]
    k0, k1 = k0_out[...], k1_out[...]
    for c, (mine, theirs) in enumerate(
        zip(target_tiles(t_mine, 1 - me), target_tiles(t_theirs, 1 - me))
    ):
        for b, tile in enumerate(by_batch(me == 0, mine, theirs)):
            at = (b * plan.col_tiles + c) * high
            outs[0][at] = outs[0][at] - tile
    gram = dot(k1, jnp.concatenate([k0] * plan.pack, 0), ((1,), (1,)))
    for q, out in enumerate(outs):
        rows = gram[q * span : (q + 1) * span]
        rows = rows.reshape(plan.gram_rows, plan.pack, each, rows.shape[1])
        lane = lax.broadcasted_iota(jnp.int32, rows.shape[:1] + rows.shape[2:], 2)
        packed = rows[:, 0]
        for i in range(1, plan.pack):
            packed = jnp.where(lane >= i * plan.width, rows[:, i], packed)
        tiles = [packed[:, :, i : i + LANES] for i in range(0, packed.shape[2], LANES)]
        for u, tile in enumerate(seen_by(plan, tiles, q)):
            at = plan.sums + u * plan.gram_rows
            out[at : at + plan.gram_rows] = tile


def quad_body(own, *refs):
    *others, out = refs
    total = own[...]
    for other in others:
        total = total + other[...]
    out[...] = total


def high_body(plan, bit, mine, other, out):
    for at in range(0, plan.sums, plan.high):
        for h in range(plan.high):
            out[at + h] = mine[at + h] + other[at + (h ^ bit)]
    t = plan.gram_rows
    step = bit // plan.pack
    for r in range(t):
        tiles = [other[plan.sums + u * t + (r ^ step)] for u in range(plan.gram_tiles)]
        if bit < plan.pack:
            tiles = xor_lanes(tiles, bit * plan.width)
        for u, tile in enumerate(xor_lanes(tiles, bit * plan.each)):
            out[plan.sums + u * t + r] = mine[plan.sums + u * t + r] + tile


def unpack(plan, packets, b):
    span = plan.high * plan.each
    rows = []
    for packet in packets:
        at = [(b * plan.col_tiles + c) * plan.high for c in range(plan.col_tiles)]
        tiles = [packet[i : i + plan.high].reshape(span, LANES) for i in at]
        rows.append(jnp.concatenate(tiles, 1))
    return jnp.concatenate(rows, 0)


def gram_of(plan, packet, q):
    t = plan.gram_rows
    tiles = [packet[plan.sums + u * t : plan.sums + (u + 1) * t] for u in range(plan.gram_tiles)]
    packed = jnp.concatenate(seen_by(plan, tiles, q), 2)
    lane = lax.broadcasted_iota(jnp.int32, packed.shape, 2) // plan.width
    return jnp.stack([jnp.where(lane == i, packed, 0.0) for i in range(plan.pack)], 1)


def chip_body(plan, rate, *refs):
    *packets, mine_out, theirs_out = refs
    packets = packets[::-1]
    half = plan.each // 2
    res0 = jnp.concatenate([unpack(plan, packets, 0)] * plan.pack, 0)
    gram = gram_of(plan, packets[0], 0)[0, 0]
    at = [(plan.col_tiles + c) * plan.high for c in range(plan.col_tiles)]
    late = jnp.concatenate([packets[0][i] for i in at], 1)
    late = late - rate * dot(gram, res0, ((1,), (0,)))
    first = lax.axis_index("row") == 0
    a, b = late[:half], late[half:]
    mine_out[...] = jnp.where(first, a, b)
    theirs_out[...] = jnp.where(first, b, a)


def update_body(plan, rate, *refs):
    k0, k1, weights, *packets, out = refs
    packets = packets[::-1]
    res0, late = unpack(plan, packets, 0), unpack(plan, packets, 1)
    grams = [gram_of(plan, packet, q) for q, packet in enumerate(packets)]
    gram = jnp.concatenate([g.reshape(-1, g.shape[-1]) for g in grams], 0)
    res1 = late - rate * dot(gram, jnp.concatenate([res0] * plan.pack, 0), ((1,), (0,)))
    grad = dot(k0[...], res0, ((0,), (0,))) + dot(k1[...], res1, ((0,), (0,)))
    out[...] = weights[...] - rate * grad


def finish_body(weights, mine, back, weights_out, residual_out, residual, sems):
    copies = [
        pltpu.make_async_copy(a, b, sems.at[i])
        for i, (a, b) in enumerate(((weights, weights_out), (residual, residual_out)))
    ]
    copies[0].start()
    first = lax.axis_index("row") == 0
    a, b = mine[...], back[...]
    cols = a.shape[1]
    residual[:, :cols] = jnp.where(first, a, b)
    residual[:, cols:] = jnp.where(first, b, a)
    copies[1].start()
    for c in copies:
        c.wait()


def per_device(dataset, centers, weights, batch_index, targets, gamma):
    shards = lax.axis_size("center")
    cores = lax.axis_size("row")
    batches, rows_here = batch_index.shape
    assert cores == 2 and batches == 2 and shards % QUAD == 0 and shards & (shards - 1) == 0
    features = dataset.shape[1]
    count, cols = weights.shape
    each = batches * rows_here
    high = shards // QUAD
    span = high * each
    n = shards * each
    width = shards * cores * rows_here
    rate = 0.5 / width
    plan = Plan(high, each, cols // LANES, width, max(1, LANES // width))
    quad = range(1, QUAD)
    bits = [1 << i for i in range(high.bit_length() - 1)]

    (local,) = call(
        pick_body,
        [kept(each, features)],
        "pick",
        (batch_index, pl.ANY),
        (dataset, pl.ANY),
        scratch_shapes=[
            pltpu.SMEM(batch_index.shape, jnp.int32),
            pltpu.VMEM(dataset.shape, jnp.float32),
            pltpu.SemaphoreType.DMA((2,)),
        ],
    )
    split, row, targets = call(
        prepare_body,
        [
            pltpu.VMEM((3, count, features), jnp.bfloat16),
            kept(8, count),
            kept(*targets.shape),
        ],
        "prepare",
        (centers, pl.ANY),
        (targets, pl.ANY),
        scratch_shapes=[
            pltpu.VMEM(centers.shape, jnp.float32),
            pltpu.SemaphoreType.DMA((2,)),
        ],
    )
    spread = jnp.broadcast_to(gamma, (8, count))
    rows = local
    for bit in bits:
        rows = jnp.concatenate([rows, across(rows, QUAD * bit)], 0)
    own = [
        call(kernel_body, [kept(span, count)], "kernel", spread, x, split, row)[0]
        for x in [rows] + [across(rows, q) for q in quad]
    ]
    own[0], weights_other, targets_other = lax.optimization_barrier(
        (own[0], swap_cores(weights), swap_cores(targets))
    )
    own = jnp.concatenate(own, 0)
    packet = (plan.tiles, each, LANES)
    swapped = swap_cores(own)
    weight_split, mine_sums = call(
        functools.partial(weights_body, plan),
        [pltpu.VMEM((2, 3, count, cols), jnp.bfloat16), kept(n, cols)],
        "weights",
        own,
        weights,
        weights_other,
    )
    k0, k1, keep, *sent = call(
        functools.partial(predict_body, plan),
        [kept(n, count)] * 2 + [kept(*packet)] * QUAD,
        "predict",
        own,
        swapped,
        mine_sums,
        weight_split,
        targets,
        targets_other,
    )
    (total,) = call(
        quad_body,
        [kept(*packet)],
        "quad",
        keep,
        *[across(sent[q - 1], q) for q in reversed(quad)],
    )
    for bit in bits:
        (total,) = call(
            functools.partial(high_body, plan, bit),
            [kept(*packet)],
            "high",
            total,
            partner(total, QUAD * bit),
        )
    packets = [across(total, q) for q in reversed(quad)] + [swap_cores(total)]
    mine, theirs = call(
        functools.partial(chip_body, plan, rate), [kept(rows_here, cols)] * 2, "chip", *packets
    )
    back = swap_cores(theirs)
    (new_weights,) = call(
        functools.partial(update_body, plan, rate),
        [kept(count, cols)],
        "update",
        k0,
        k1,
        weights,
        *packets,
    )
    new_weights, residual = call(
        finish_body,
        [stored(count, cols), stored(rows_here, 2 * cols)],
        "finish",
        new_weights,
        mine,
        back,
        out_space=pl.ANY,
        scratch_shapes=[
            pltpu.VMEM((rows_here, 2 * cols), jnp.float32),
            pltpu.SemaphoreType.DMA((2,)),
        ],
    )
    return (new_weights, residual)


def solution(mesh):
    return jax.shard_map(
        per_device,
        mesh=mesh,
        in_specs=(
            P(("groups", "center", "row"), None),
            P(("groups", "center"), None),
            P(("groups", "center"), "row"),
            P(None, ("groups", "center", "row")),
            P(None, ("groups", "center", "row"), None),
            P("groups"),
        ),
        out_specs=(P(("groups", "center"), "row"), P(("groups", "center", "row"), None)),
        check_vma=False,
    )
```

```python
import functools
import math
from typing import NamedTuple

import jax
import jax.numpy as jnp
from jax import lax
from jax.experimental import pallas as pl
from jax.experimental.pallas import tpu as pltpu
from jax.sharding import PartitionSpec as P

LANES = 128
QUAD = 4
KEPT_BYTES = 400 << 10


class Plan(NamedTuple):
    high: int
    each: int
    col_tiles: int
    width: int
    pack: int

    @property
    def chips(self):
        return self.width // self.each

    @property
    def sums(self):
        return self.col_tiles * self.high

    @property
    def gram_rows(self):
        return self.chips // 2 // self.pack

    @property
    def gram_cols(self):
        return self.width * self.pack // LANES

    @property
    def grams(self):
        return self.gram_rows * self.gram_cols

    @property
    def tiles(self):
        return self.sums + self.grams

    def blocks(self):
        for q in range(QUAD):
            for h in range(self.high):
                yield q, h, int(q > 0) ^ (h.bit_count() & 1)


def dot(a, b, contract):
    return lax.dot_general(
        a,
        b,
        (contract, ((), ())),
        precision=lax.Precision.HIGHEST,
        preferred_element_type=jnp.float32,
    )


def small(x):
    bytes_each = jnp.dtype(x.dtype).itemsize
    return bytes_each == 2 or math.prod(x.shape) * bytes_each <= KEPT_BYTES


def call(body, outs, name, *args, out_space=pltpu.VMEM, **kwargs):
    args = [a if isinstance(a, tuple) else (a, pltpu.VMEM) for a in args]
    return pl.pallas_call(
        body,
        out_shape=outs,
        in_specs=[pl.BlockSpec(memory_space=space) for _, space in args],
        out_specs=[pl.BlockSpec(memory_space=out_space)] * len(outs),
        name=name,
        **kwargs,
    )(
        *[
            pltpu.with_memory_space_constraint(a, space)
            if space == pltpu.VMEM and small(a)
            else a
            for a, space in args
        ]
    )


def stored(*shape):
    return jax.ShapeDtypeStruct(shape, jnp.float32)


def kept(*shape):
    return pltpu.VMEM(shape, jnp.float32) if small(stored(*shape)) else stored(*shape)


def swap_cores(x):
    return lax.ppermute(x, "row", [(0, 1), (1, 0)])


def partner(x, bits):
    return lax.ppermute(x, "center", [(i, i ^ bits) for i in range(lax.axis_size("center"))])


def across(x, bits):
    pairs = [
        (2 * i + core, 2 * (i ^ bits) + 1 - core)
        for i in range(lax.axis_size("center"))
        for core in range(2)
    ]
    return lax.ppermute(x, ("center", "row"), pairs)


def pick_body(index, dataset, out, index_s, data, sems):
    copies = [
        pltpu.make_async_copy(a, b, sems.at[i])
        for i, (a, b) in enumerate(((index, index_s), (dataset, data)))
    ]
    for c in copies:
        c.start()
    for c in copies:
        c.wait()
    batches, count = index.shape
    for b in range(batches):
        for j in range(count):
            at = b * count + j
            out[at : at + 1] = data[pl.ds(index_s[b, j], 1), :]


def parts(x):
    out = []
    for _ in range(3):
        out.append(x.astype(jnp.bfloat16))
        x = x - out[-1].astype(jnp.float32)
    return out


def parts_dot(left, right, axis):
    n = left[0].shape[0]
    total = 0.0
    for i in (2, 1, 0):
        part = lax.dot_general(
            jnp.concatenate(left[: 3 - i], 0),
            right[i],
            (((1,), (axis,)), ((), ())),
            preferred_element_type=jnp.float32,
        )
        for j in reversed(range(3 - i)):
            total = total + part[j * n : (j + 1) * n]
    return total


def prepare_body(centers, split_out, row_out, held, sem):
    copy = pltpu.make_async_copy(centers, held, sem)
    copy.start()
    copy.wait()
    c = held[...]
    for i, part in enumerate(parts(c)):
        split_out[i] = part
    sq = jnp.sum(c * c, axis=1, keepdims=True)
    row_out[...] = jnp.broadcast_to(sq, (c.shape[0], LANES)).T[: row_out.shape[0]]


def weights_body(mine, theirs, split_out):
    first = lax.axis_index("row") == 0
    a, b = mine[...], theirs[...]
    cols = a.shape[1]
    for side, w in enumerate((jnp.where(first, a, b), jnp.where(first, b, a))):
        for i, part in enumerate(parts(w)):
            split_out[i, :, side * cols : (side + 1) * cols] = part


def block_body(plan, gamma, rows, split, row, weights, *refs):
    *targets, k_out, out = refs
    x = rows[...]
    row_sq = jnp.sum(x * x, axis=1, keepdims=True)
    cross = parts_dot(parts(x), split, 1)
    k = jnp.exp(-gamma[:1] * (row_sq + row[:1] - 2.0 * cross))
    k_out[...] = k
    part = parts_dot(parts(k), weights, 0)
    high = plan.high
    for c in range(plan.col_tiles):
        tile = part[:, c * LANES : (c + 1) * LANES]
        out[c * high : (c + 1) * high] = tile.reshape(high, plan.each, LANES)
    for t in targets:
        wanted = jnp.concatenate([t[b] for b in range(t.shape[0])], 0)
        for c in range(plan.col_tiles):
            out[c * high] = out[c * high] - wanted[:, c * LANES : (c + 1) * LANES]


def by_batch(is_first, mine, theirs):
    first, second = jnp.where(is_first, mine, theirs), jnp.where(is_first, theirs, mine)
    half = mine.shape[0] // 2
    low = lax.broadcasted_iota(jnp.int32, mine.shape, 0) < half
    return (
        jnp.where(low, first, pltpu.roll(second, half, 0)),
        jnp.where(low, pltpu.roll(first, half, 0), second),
    )


def chip_at(q, h):
    return lax.axis_index("center") ^ (QUAD * h + q)


def gram_body(plan, own, swapped, k0_out, k1_out, keep, send):
    each = plan.each
    me = lax.axis_index("row")
    for q, h, crossed in plan.blocks():
        at = (q * plan.high + h) * each
        tile = slice(at, at + each)
        to = pl.ds(pl.multiple_of(chip_at(q, h) * each, each), each)
        k0_out[to], k1_out[to] = by_batch(me == crossed, own[tile], swapped[tile])
    k0 = jnp.concatenate([k0_out[...]] * plan.pack, 0)
    gram = dot(k1_out[...], k0, ((1,), (1,)))
    gram = gram.reshape(plan.chips // 2, 2, each, gram.shape[1])
    even, odd = gram[:, 0], gram[:, 1]
    half = each // 2
    low = lax.broadcasted_iota(jnp.int32, even.shape, 1) < half
    core0 = jnp.where(low, even, pltpu.roll(odd, half, 1))
    core1 = jnp.where(low, pltpu.roll(even, half, 1), odd)
    t = plan.gram_rows
    lane = lax.broadcasted_iota(jnp.int32, (t,) + even.shape[1:], 2)
    sides = []
    for core in (core0, core1):
        packed = core[:t]
        for i in range(1, plan.pack):
            packed = jnp.where(lane >= i * plan.width, core[i * t : (i + 1) * t], packed)
        sides.append(packed)
    first = me == 0
    for out, x in (
        (keep, jnp.where(first, sides[0], sides[1])),
        (send, jnp.where(first, sides[1], sides[0])),
    ):
        for u in range(plan.gram_cols):
            out[u * t : (u + 1) * t] = x[:, :, u * LANES : (u + 1) * LANES]


def quad_body(plan, *refs):
    *sums, gram, out = refs
    total = sums[0][...]
    for other in sums[1:]:
        total = total + other[...]
    out[: plan.sums] = total
    out[plan.sums :] = gram[...]


def high_body(plan, bit, mine, gram, other, out):
    for at in range(0, plan.sums, plan.high):
        for h in range(plan.high):
            out[at + h] = mine[at + h] + other[at + (h ^ bit)]
    out[plan.sums :] = gram[...] + other[plan.sums :]


def solve_body(plan, rate, *refs):
    mine, refs = refs[:QUAD][::-1], refs[QUAD:]
    theirs, refs = refs[:QUAD][::-1], refs[QUAD:]
    k0, k1, weights, weights_out, residual_out, res0, res1, weights_new, residual, sems = refs
    each, high = plan.each, plan.high
    half = each // 2
    me = lax.axis_index("row")
    for q, h, crossed in plan.blocks():
        to = pl.ds(pl.multiple_of(chip_at(q, h) * each, each), each)
        for c in range(plan.col_tiles):
            at = c * high + h
            cols = slice(c * LANES, (c + 1) * LANES)
            res0[to, cols], res1[to, cols] = by_batch(me == crossed, mine[q][at], theirs[q][at])
    grams = lambda packet: packet[plan.sums :]
    here = grams(mine[0]) + grams(theirs[1]) + grams(theirs[2]) + grams(theirs[3])
    there = grams(theirs[0]) + grams(mine[1]) + grams(mine[2]) + grams(mine[3])
    first = me == 0
    t = plan.gram_rows
    rows = []
    for x in (jnp.where(first, here, there), jnp.where(first, there, here)):
        x = jnp.concatenate([x[u * t : (u + 1) * t] for u in range(plan.gram_cols)], 2)
        lane = lax.broadcasted_iota(jnp.int32, x.shape, 2) // plan.width
        rows += [jnp.where(lane == i, x, 0.0) for i in range(plan.pack)]
    gram = jnp.concatenate(rows, 0)
    gram = gram.reshape(-1, gram.shape[2])
    step = dot(gram, jnp.concatenate([res0[...]] * plan.pack, 0), ((1,), (0,))) * rate
    core0, core1 = (
        x.reshape(plan.chips // 2, each, -1) for x in (step[: plan.width // 2], step[plan.width // 2 :])
    )
    low = lax.broadcasted_iota(jnp.int32, core0.shape, 1) < half
    even = jnp.where(low, core0, pltpu.roll(core1, half, 1))
    odd = jnp.where(low, pltpu.roll(core0, half, 1), core1)
    res1[...] = res1[...] - jnp.stack([even, odd], 1).reshape(res1.shape)
    tile = res1[pl.ds(pl.multiple_of(lax.axis_index("center") * each, each), each), :]
    residual[...] = jnp.where(first, tile[:half], tile[half:])
    copies = [
        pltpu.make_async_copy(a, b, sems.at[i])
        for i, (a, b) in enumerate(((residual, residual_out), (weights_new, weights_out)))
    ]
    copies[0].start()
    cols = weights.shape[1]
    side = lambda x: jnp.where(first, x[:, :cols], x[:, cols:])
    grad = dot(k0[...], side(res0[...]), ((0,), (0,))) + dot(
        k1[...], side(res1[...]), ((0,), (0,))
    )
    weights_new[...] = weights[...] - rate * grad
    copies[1].start()
    for c in copies:
        c.wait()


def per_device(dataset, centers, weights, batch_index, targets, gamma):
    shards = lax.axis_size("center")
    cores = lax.axis_size("row")
    batches, rows_here = batch_index.shape
    assert cores == 2 and batches == 2 and shards % QUAD == 0 and shards & (shards - 1) == 0
    features = dataset.shape[1]
    count, cols = weights.shape
    each = batches * rows_here
    high = shards // QUAD
    span = high * each
    n = shards * each
    width = shards * cores * rows_here
    rate = 0.5 / width
    plan = Plan(high, each, 2 * cols // LANES, width, max(1, LANES // width))
    quad = range(1, QUAD)
    bits = [1 << i for i in range(high.bit_length() - 1)]

    (local,) = call(
        pick_body,
        [kept(each, features)],
        "pick",
        (batch_index, pl.ANY),
        (dataset, pl.ANY),
        scratch_shapes=[
            pltpu.SMEM(batch_index.shape, jnp.int32),
            pltpu.VMEM(dataset.shape, jnp.float32),
            pltpu.SemaphoreType.DMA((2,)),
        ],
    )
    split, row = call(
        prepare_body,
        [pltpu.VMEM((3, count, features), jnp.bfloat16), kept(8, count)],
        "prepare",
        (centers, pl.ANY),
        scratch_shapes=[pltpu.VMEM(centers.shape, jnp.float32), pltpu.SemaphoreType.DMA],
    )
    spread = jnp.broadcast_to(gamma, (8, count))
    (weight_split,) = call(
        weights_body,
        [pltpu.VMEM((3, count, 2 * cols), jnp.bfloat16)],
        "weights",
        weights,
        swap_cores(weights),
    )
    rows = local
    for bit in bits:
        rows = jnp.concatenate([rows, across(rows, QUAD * bit)], 0)
    own, packets = [], []
    for q, x in enumerate([rows] + [across(rows, q) for q in quad]):
        k, packet = call(
            functools.partial(block_body, plan),
            [kept(span, count), kept(plan.sums, each, LANES)],
            "block",
            spread,
            x,
            split,
            row,
            weight_split,
            *([targets] if q == 0 else []),
        )
        own.append(k)
        packets.append(packet)
    sums = [across(packets[q], q) for q in reversed(quad)]
    own = jnp.concatenate(own, 0)
    k0, k1, gram, gram_sent = call(
        functools.partial(gram_body, plan),
        [kept(n, count)] * 2 + [kept(plan.grams, each, LANES)] * 2,
        "gram",
        own,
        swap_cores(own),
    )
    shape = kept(plan.tiles, each, LANES)
    (total,) = call(
        functools.partial(quad_body, plan), [shape], "quad", packets[0], *sums, gram_sent
    )
    for i, bit in enumerate(bits):
        if i == 0:
            other = across(total, QUAD * bit)
        else:
            gram = total[plan.sums :]
            other = jnp.concatenate(
                [across(total[: plan.sums], QUAD * bit), partner(gram, QUAD * bit)], 0
            )
        (total,) = call(
            functools.partial(high_body, plan, bit), [shape], "high", total, gram, other
        )
    mine = [across(total, q) for q in reversed(quad)] + [total]
    new_weights, residual = call(
        functools.partial(solve_body, plan, rate),
        [stored(count, cols), stored(rows_here, 2 * cols)],
        "solve",
        *mine,
        *[swap_cores(x) for x in mine],
        k0,
        k1,
        weights,
        out_space=pl.ANY,
        scratch_shapes=[
            pltpu.VMEM((width, 2 * cols), jnp.float32),
            pltpu.VMEM((width, 2 * cols), jnp.float32),
            pltpu.VMEM((count, cols), jnp.float32),
            pltpu.VMEM((rows_here, 2 * cols), jnp.float32),
            pltpu.SemaphoreType.DMA((2,)),
        ],
    )
    return (new_weights, residual)


def solution(mesh):
    return jax.shard_map(
        per_device,
        mesh=mesh,
        in_specs=(
            P(("groups", "center", "row"), None),
            P(("groups", "center"), None),
            P(("groups", "center"), "row"),
            P(None, ("groups", "center", "row")),
            P(None, ("groups", "center", "row"), None),
            P("groups"),
        ),
        out_specs=(P(("groups", "center"), "row"), P(("groups", "center", "row"), None)),
        check_vma=False,
    )
```

```python
import functools
import math
from typing import NamedTuple

import jax
import jax.numpy as jnp
from jax import lax
from jax.experimental import pallas as pl
from jax.experimental.pallas import tpu as pltpu
from jax.sharding import PartitionSpec as P


LANES = 128
QUAD = 4
KEPT_BYTES = 400 << 10


class Plan(NamedTuple):
    high: int
    each: int
    col_tiles: int
    width: int
    pack: int

    @property
    def chips(self):
        return self.width // self.each

    @property
    def sums(self):
        return self.col_tiles * self.high

    @property
    def gram_rows(self):
        return self.chips // 2 // self.pack

    @property
    def gram_cols(self):
        return self.width * self.pack // LANES

    @property
    def grams(self):
        return self.gram_rows * self.gram_cols

    @property
    def tiles(self):
        return self.sums + self.grams

    def blocks(self):
        for q in range(QUAD):
            for h in range(self.high):
                yield q, h, int(q > 0) ^ (h.bit_count() & 1)


def dot(a, b, contract):
    return lax.dot_general(
        a,
        b,
        (contract, ((), ())),
        precision=lax.Precision.HIGHEST,
        preferred_element_type=jnp.float32,
    )


def small(x):
    bytes_each = jnp.dtype(x.dtype).itemsize
    return bytes_each == 2 or math.prod(x.shape) * bytes_each <= KEPT_BYTES


def call(body, outs, *args, out_space=pltpu.VMEM, **kwargs):
    args = [a if isinstance(a, tuple) else (a, pltpu.VMEM) for a in args]
    return pl.pallas_call(
        body,
        out_shape=outs,
        in_specs=[pl.BlockSpec(memory_space=space) for _, space in args],
        out_specs=[pl.BlockSpec(memory_space=out_space)] * len(outs),
        **kwargs,
    )(
        *[
            pltpu.with_memory_space_constraint(a, space)
            if space == pltpu.VMEM and small(a)
            else a
            for a, space in args
        ]
    )


def stored(*shape):
    return jax.ShapeDtypeStruct(shape, jnp.float32)


def kept(*shape):
    return pltpu.VMEM(shape, jnp.float32) if small(stored(*shape)) else stored(*shape)


def swap_cores(x):
    return lax.ppermute(x, "row", [(0, 1), (1, 0)])


def partner(x, bits):
    return lax.ppermute(x, "center", [(i, i ^ bits) for i in range(lax.axis_size("center"))])


def across(x, bits):
    pairs = [
        (2 * i + core, 2 * (i ^ bits) + 1 - core)
        for i in range(lax.axis_size("center"))
        for core in range(2)
    ]
    return lax.ppermute(x, ("center", "row"), pairs)


def pick_body(index, dataset, out, index_s, data, sems):
    copies = [
        pltpu.make_async_copy(a, b, sems.at[i])
        for i, (a, b) in enumerate(((index, index_s), (dataset, data)))
    ]
    for c in copies:
        c.start()
    for c in copies:
        c.wait()
    batches, count = index.shape
    for b in range(batches):
        for j in range(count):
            at = b * count + j
            out[at : at + 1] = data[pl.ds(index_s[b, j], 1), :]


def parts(x):
    out = []
    for _ in range(3):
        out.append(x.astype(jnp.bfloat16))
        x = x - out[-1].astype(jnp.float32)
    return out


def parts_dot(left, right, axis):
    n = left[0].shape[0]
    total = 0.0
    for i in (2, 1, 0):
        part = lax.dot_general(
            jnp.concatenate(left[: 3 - i], 0),
            right[i],
            (((1,), (axis,)), ((), ())),
            preferred_element_type=jnp.float32,
        )
        for j in reversed(range(3 - i)):
            total = total + part[j * n : (j + 1) * n]
    return total


def prepare_body(centers, split_out, row_out, held, sem):
    copy = pltpu.make_async_copy(centers, held, sem)
    copy.start()
    copy.wait()
    c = held[...]
    for i, part in enumerate(parts(c)):
        split_out[i] = part
    sq = jnp.sum(c * c, axis=1, keepdims=True)
    row_out[...] = jnp.broadcast_to(sq, (c.shape[0], LANES)).T[: row_out.shape[0]]


def weights_body(mine, theirs, split_out):
    first = lax.axis_index("row") == 0
    a, b = mine[...], theirs[...]
    cols = a.shape[1]
    for side, w in enumerate((jnp.where(first, a, b), jnp.where(first, b, a))):
        for i, part in enumerate(parts(w)):
            split_out[i, :, side * cols : (side + 1) * cols] = part


def block_body(plan, members, gamma, split, row, weights, *refs):
    rows, refs = refs[:members], refs[members:]
    targets, outs = refs[: -2 * members], refs[-2 * members :]
    x = jnp.concatenate([r[...] for r in rows], 0)
    row_sq = jnp.sum(x * x, axis=1, keepdims=True)
    cross = parts_dot(parts(x), split, 1)
    k = jnp.exp(-gamma[:1] * (row_sq + row[:1] - 2.0 * cross))
    part = parts_dot(parts(k), weights, 0)
    high = plan.high
    span = high * plan.each
    for i in range(members):
        k_out, out = outs[i], outs[members + i]
        k_out[...] = k[i * span : (i + 1) * span]
        for c in range(plan.col_tiles):
            tile = part[i * span : (i + 1) * span, c * LANES : (c + 1) * LANES]
            out[c * high : (c + 1) * high] = tile.reshape(high, plan.each, LANES)
    for t in targets:
        wanted = jnp.concatenate([t[b] for b in range(t.shape[0])], 0)
        for c in range(plan.col_tiles):
            outs[members][c * high] = (
                outs[members][c * high] - wanted[:, c * LANES : (c + 1) * LANES]
            )


def by_batch(is_first, mine, theirs):
    first, second = jnp.where(is_first, mine, theirs), jnp.where(is_first, theirs, mine)
    half = mine.shape[0] // 2
    low = lax.broadcasted_iota(jnp.int32, mine.shape, 0) < half
    return (
        jnp.where(low, first, pltpu.roll(second, half, 0)),
        jnp.where(low, pltpu.roll(first, half, 0), second),
    )


def chip_at(q, h):
    return lax.axis_index("center") ^ (QUAD * h + q)


def gram_body(plan, own, swapped, k0_out, k1_out, keep, send):
    each = plan.each
    me = lax.axis_index("row")
    for q, h, crossed in plan.blocks():
        at = (q * plan.high + h) * each
        tile = slice(at, at + each)
        to = pl.ds(pl.multiple_of(chip_at(q, h) * each, each), each)
        k0_out[to], k1_out[to] = by_batch(me == crossed, own[tile], swapped[tile])
    k0 = jnp.concatenate([k0_out[...]] * plan.pack, 0)
    gram = dot(k1_out[...], k0, ((1,), (1,)))
    gram = gram.reshape(plan.chips // 2, 2, each, gram.shape[1])
    even, odd = gram[:, 0], gram[:, 1]
    half = each // 2
    low = lax.broadcasted_iota(jnp.int32, even.shape, 1) < half
    core0 = jnp.where(low, even, pltpu.roll(odd, half, 1))
    core1 = jnp.where(low, pltpu.roll(even, half, 1), odd)
    t = plan.gram_rows
    lane = lax.broadcasted_iota(jnp.int32, (t,) + even.shape[1:], 2)
    sides = []
    for core in (core0, core1):
        packed = core[:t]
        for i in range(1, plan.pack):
            packed = jnp.where(lane >= i * plan.width, core[i * t : (i + 1) * t], packed)
        sides.append(packed)
    first = me == 0
    for out, x in (
        (keep, jnp.where(first, sides[0], sides[1])),
        (send, jnp.where(first, sides[1], sides[0])),
    ):
        for u in range(plan.gram_cols):
            out[u * t : (u + 1) * t] = x[:, :, u * LANES : (u + 1) * LANES]


def quad_body(plan, *refs):
    *sums, gram, out = refs
    total = sums[0][...]
    for other in sums[1:]:
        total = total + other[...]
    out[: plan.sums] = total
    out[plan.sums :] = gram[...]


def high_body(plan, bit, mine, gram, other, out):
    for at in range(0, plan.sums, plan.high):
        for h in range(plan.high):
            out[at + h] = mine[at + h] + other[at + (h ^ bit)]
    out[plan.sums :] = gram[...] + other[plan.sums :]


def solve_body(plan, rate, *refs):
    mine, refs = refs[:QUAD][::-1], refs[QUAD:]
    theirs, refs = refs[:QUAD][::-1], refs[QUAD:]
    k0, k1, weights, weights_out, residual_out, res0, res1, weights_new, residual, sems = refs
    each, high = plan.each, plan.high
    half = each // 2
    me = lax.axis_index("row")
    for q, h, crossed in plan.blocks():
        to = pl.ds(pl.multiple_of(chip_at(q, h) * each, each), each)
        for c in range(plan.col_tiles):
            at = c * high + h
            cols = slice(c * LANES, (c + 1) * LANES)
            res0[to, cols], res1[to, cols] = by_batch(me == crossed, mine[q][at], theirs[q][at])
    grams = lambda packet: packet[plan.sums :]
    here = grams(mine[0]) + grams(theirs[1]) + grams(theirs[2]) + grams(theirs[3])
    there = grams(theirs[0]) + grams(mine[1]) + grams(mine[2]) + grams(mine[3])
    first = me == 0
    t = plan.gram_rows
    rows = []
    for x in (jnp.where(first, here, there), jnp.where(first, there, here)):
        x = jnp.concatenate([x[u * t : (u + 1) * t] for u in range(plan.gram_cols)], 2)
        lane = lax.broadcasted_iota(jnp.int32, x.shape, 2) // plan.width
        rows += [jnp.where(lane == i, x, 0.0) for i in range(plan.pack)]
    gram = jnp.concatenate(rows, 0)
    gram = gram.reshape(-1, gram.shape[2])
    step = dot(gram, jnp.concatenate([res0[...]] * plan.pack, 0), ((1,), (0,))) * rate
    core0, core1 = (
        x.reshape(plan.chips // 2, each, -1) for x in (step[: plan.width // 2], step[plan.width // 2 :])
    )
    low = lax.broadcasted_iota(jnp.int32, core0.shape, 1) < half
    even = jnp.where(low, core0, pltpu.roll(core1, half, 1))
    odd = jnp.where(low, pltpu.roll(core0, half, 1), core1)
    res1[...] = res1[...] - jnp.stack([even, odd], 1).reshape(res1.shape)
    tile = res1[pl.ds(pl.multiple_of(lax.axis_index("center") * each, each), each), :]
    residual[...] = jnp.where(first, tile[:half], tile[half:])
    copies = [
        pltpu.make_async_copy(a, b, sems.at[i])
        for i, (a, b) in enumerate(((residual, residual_out), (weights_new, weights_out)))
    ]
    copies[0].start()
    cols = weights.shape[1]
    side = lambda x: jnp.where(first, x[:, :cols], x[:, cols:])
    grad = dot(k0[...], side(res0[...]), ((0,), (0,))) + dot(
        k1[...], side(res1[...]), ((0,), (0,))
    )
    weights_new[...] = weights[...] - rate * grad
    copies[1].start()
    for c in copies:
        c.wait()


def body(dataset, centers, weights, batch_index, targets, gamma):
    shards = lax.axis_size("center")
    cores = lax.axis_size("row")
    batches, rows_here = batch_index.shape
    assert cores == 2 and batches == 2 and shards % QUAD == 0 and shards & (shards - 1) == 0
    features = dataset.shape[1]
    count, cols = weights.shape
    each = batches * rows_here
    high = shards // QUAD
    span = high * each
    n = shards * each
    width = shards * cores * rows_here
    rate = 0.5 / width
    plan = Plan(high, each, 2 * cols // LANES, width, max(1, LANES // width))
    quad = range(1, QUAD)
    bits = [1 << i for i in range(high.bit_length() - 1)]

    (local,) = call(
        pick_body,
        [kept(each, features)],
        (batch_index, pl.ANY),
        (dataset, pl.ANY),
        scratch_shapes=[
            pltpu.SMEM(batch_index.shape, jnp.int32),
            pltpu.VMEM(dataset.shape, jnp.float32),
            pltpu.SemaphoreType.DMA((2,)),
        ],
    )
    split, row = call(
        prepare_body,
        [pltpu.VMEM((3, count, features), jnp.bfloat16), kept(8, count)],
        (centers, pl.ANY),
        scratch_shapes=[pltpu.VMEM(centers.shape, jnp.float32), pltpu.SemaphoreType.DMA],
    )
    spread = jnp.broadcast_to(gamma, (8, count))
    (weight_split,) = call(
        weights_body, [pltpu.VMEM((3, count, 2 * cols), jnp.bfloat16)], weights, swap_cores(weights)
    )
    rows = local
    for bit in bits:
        rows = jnp.concatenate([rows, across(rows, QUAD * bit)], 0)
    received = [rows] + [across(rows, q) for q in quad]
    own, packets = [None] * QUAD, [None] * QUAD
    for group in ((0,), (3,), (2, 1)):
        done = call(
            functools.partial(block_body, plan, len(group)),
            [kept(span, count)] * len(group)
            + [kept(plan.sums, each, LANES)] * len(group),
            spread,
            split,
            row,
            weight_split,
            *[received[q] for q in group],
            *([targets] if group == (0,) else []),
        )
        for i, q in enumerate(group):
            own[q], packets[q] = done[i], done[len(group) + i]
    sums = [across(packets[q], q) for q in reversed(quad)]
    own = jnp.concatenate(own, 0)
    k0, k1, gram, gram_sent = call(
        functools.partial(gram_body, plan),
        [kept(n, count)] * 2 + [kept(plan.grams, each, LANES)] * 2,
        own,
        swap_cores(own),
    )
    shape = kept(plan.tiles, each, LANES)
    (total,) = call(functools.partial(quad_body, plan), [shape], packets[0], *sums, gram_sent)
    for i, bit in enumerate(bits):
        if i == 0:
            other = across(total, QUAD * bit)
        else:
            gram = total[plan.sums :]
            other = jnp.concatenate(
                [across(total[: plan.sums], QUAD * bit), partner(gram, QUAD * bit)], 0
            )
        (total,) = call(functools.partial(high_body, plan, bit), [shape], total, gram, other)
    mine = [across(total, q) for q in reversed(quad)] + [total]
    new_weights, residual = call(
        functools.partial(solve_body, plan, rate),
        [stored(count, cols), stored(rows_here, 2 * cols)],
        *mine,
        *[swap_cores(x) for x in mine],
        k0,
        k1,
        weights,
        out_space=pl.ANY,
        scratch_shapes=[
            pltpu.VMEM((width, 2 * cols), jnp.float32),
            pltpu.VMEM((width, 2 * cols), jnp.float32),
            pltpu.VMEM((count, cols), jnp.float32),
            pltpu.VMEM((rows_here, 2 * cols), jnp.float32),
            pltpu.SemaphoreType.DMA((2,)),
        ],
    )
    return (new_weights, residual)


def solution(mesh):
    return jax.shard_map(
        body,
        mesh=mesh,
        in_specs=(
            P(("groups", "center", "row"), None),
            P(("groups", "center"), None),
            P(("groups", "center"), "row"),
            P(None, ("groups", "center", "row")),
            P(None, ("groups", "center", "row"), None),
            P("groups"),
        ),
        out_specs=(P(("groups", "center"), "row"), P(("groups", "center", "row"), None)),
        check_vma=False,
    )
```

```python
import functools
import math
from typing import NamedTuple

import jax
import jax.numpy as jnp
from jax import lax
from jax.experimental import pallas as pl
from jax.experimental.pallas import tpu as pltpu
from jax.sharding import PartitionSpec as P


LANES = 128
QUAD = 4
KEPT_BYTES = 400 << 10


class Plan(NamedTuple):
    high: int
    each: int
    col_tiles: int
    width: int
    pack: int

    @property
    def chips(self):
        return self.width // self.each

    @property
    def sums(self):
        return self.col_tiles * self.high

    @property
    def gram_rows(self):
        return self.chips // 2 // self.pack

    @property
    def gram_cols(self):
        return self.width * self.pack // LANES

    @property
    def grams(self):
        return self.gram_rows * self.gram_cols

    @property
    def tiles(self):
        return self.sums + self.grams

    def blocks(self):
        for q in range(QUAD):
            for h in range(self.high):
                yield q, h, int(q > 0) ^ (h.bit_count() & 1)


def dot(a, b, contract):
    return lax.dot_general(
        a,
        b,
        (contract, ((), ())),
        precision=lax.Precision.HIGHEST,
        preferred_element_type=jnp.float32,
    )


def small(x):
    bytes_each = jnp.dtype(x.dtype).itemsize
    return bytes_each == 2 or math.prod(x.shape) * bytes_each <= KEPT_BYTES


def call(body, outs, *args, out_space=pltpu.VMEM, **kwargs):
    args = [a if isinstance(a, tuple) else (a, pltpu.VMEM) for a in args]
    return pl.pallas_call(
        body,
        out_shape=outs,
        in_specs=[pl.BlockSpec(memory_space=space) for _, space in args],
        out_specs=[pl.BlockSpec(memory_space=out_space)] * len(outs),
        **kwargs,
    )(
        *[
            pltpu.with_memory_space_constraint(a, space)
            if space == pltpu.VMEM and small(a)
            else a
            for a, space in args
        ]
    )


def stored(*shape):
    return jax.ShapeDtypeStruct(shape, jnp.float32)


def kept(*shape):
    return pltpu.VMEM(shape, jnp.float32) if small(stored(*shape)) else stored(*shape)


def swap_cores(x):
    return lax.ppermute(x, "row", [(0, 1), (1, 0)])


def partner(x, bits):
    return lax.ppermute(x, "center", [(i, i ^ bits) for i in range(lax.axis_size("center"))])


def across(x, bits):
    pairs = [
        (2 * i + core, 2 * (i ^ bits) + 1 - core)
        for i in range(lax.axis_size("center"))
        for core in range(2)
    ]
    return lax.ppermute(x, ("center", "row"), pairs)


def pick_body(index, dataset, out, index_s, data, sems):
    copies = [
        pltpu.make_async_copy(a, b, sems.at[i])
        for i, (a, b) in enumerate(((index, index_s), (dataset, data)))
    ]
    for c in copies:
        c.start()
    for c in copies:
        c.wait()
    batches, count = index.shape
    for b in range(batches):
        for j in range(count):
            at = b * count + j
            out[at : at + 1] = data[pl.ds(index_s[b, j], 1), :]


def parts(x):
    out = []
    for _ in range(3):
        out.append(x.astype(jnp.bfloat16))
        x = x - out[-1].astype(jnp.float32)
    return out


def parts_dot(left, right, axis):
    n = left[0].shape[0]
    total = 0.0
    for i in (2, 1, 0):
        part = lax.dot_general(
            jnp.concatenate(left[: 3 - i], 0),
            right[i],
            (((1,), (axis,)), ((), ())),
            preferred_element_type=jnp.float32,
        )
        for j in reversed(range(3 - i)):
            total = total + part[j * n : (j + 1) * n]
    return total


def prepare_body(centers, split_out, row_out, held, sem):
    copy = pltpu.make_async_copy(centers, held, sem)
    copy.start()
    copy.wait()
    c = held[...]
    for i, part in enumerate(parts(c)):
        split_out[i] = part
    sq = jnp.sum(c * c, axis=1, keepdims=True)
    row_out[...] = jnp.broadcast_to(sq, (c.shape[0], LANES)).T[: row_out.shape[0]]


def weights_body(mine, theirs, split_out):
    first = lax.axis_index("row") == 0
    a, b = mine[...], theirs[...]
    cols = a.shape[1]
    for side, w in enumerate((jnp.where(first, a, b), jnp.where(first, b, a))):
        for i, part in enumerate(parts(w)):
            split_out[i, :, side * cols : (side + 1) * cols] = part


def block_body(plan, members, gamma, split, row, weights, *refs):
    rows, refs = refs[:members], refs[members:]
    targets, outs = refs[: -2 * members], refs[-2 * members :]
    x = jnp.concatenate([r[...] for r in rows], 0)
    row_sq = jnp.sum(x * x, axis=1, keepdims=True)
    cross = parts_dot(parts(x), split, 1)
    k = jnp.exp(-gamma[:1] * (row_sq + row[:1] - 2.0 * cross))
    part = parts_dot(parts(k), weights, 0)
    high = plan.high
    span = high * plan.each
    for i in range(members):
        k_out, out = outs[i], outs[members + i]
        k_out[...] = k[i * span : (i + 1) * span]
        for c in range(plan.col_tiles):
            tile = part[i * span : (i + 1) * span, c * LANES : (c + 1) * LANES]
            out[c * high : (c + 1) * high] = tile.reshape(high, plan.each, LANES)
    for t in targets:
        wanted = jnp.concatenate([t[b] for b in range(t.shape[0])], 0)
        for c in range(plan.col_tiles):
            outs[members][c * high] = (
                outs[members][c * high] - wanted[:, c * LANES : (c + 1) * LANES]
            )


def by_batch(is_first, mine, theirs):
    first, second = jnp.where(is_first, mine, theirs), jnp.where(is_first, theirs, mine)
    half = mine.shape[0] // 2
    low = lax.broadcasted_iota(jnp.int32, mine.shape, 0) < half
    return (
        jnp.where(low, first, pltpu.roll(second, half, 0)),
        jnp.where(low, pltpu.roll(first, half, 0), second),
    )


def chip_at(q, h):
    return lax.axis_index("center") ^ (QUAD * h + q)


def gram_body(plan, own, swapped, turned, keep, send, k0_out, k1_out):
    each = plan.each
    me = lax.axis_index("row")
    for q, h, crossed in plan.blocks():
        at = (q * plan.high + h) * each
        tile = slice(at, at + each)
        to = pl.ds(pl.multiple_of(chip_at(q, h) * each, each), each)
        k0_out[to], k1_out[to] = by_batch(me == crossed, own[tile], swapped[tile])
    turned[...] = jnp.concatenate([k0_out[...], k1_out[...]], 0).T
    k0 = jnp.concatenate([k0_out[...]] * plan.pack, 0)
    gram = dot(k1_out[...], k0, ((1,), (1,)))
    gram = gram.reshape(plan.chips // 2, 2, each, gram.shape[1])
    even, odd = gram[:, 0], gram[:, 1]
    half = each // 2
    low = lax.broadcasted_iota(jnp.int32, even.shape, 1) < half
    core0 = jnp.where(low, even, pltpu.roll(odd, half, 1))
    core1 = jnp.where(low, pltpu.roll(even, half, 1), odd)
    t = plan.gram_rows
    lane = lax.broadcasted_iota(jnp.int32, (t,) + even.shape[1:], 2)
    sides = []
    for core in (core0, core1):
        packed = core[:t]
        for i in range(1, plan.pack):
            packed = jnp.where(lane >= i * plan.width, core[i * t : (i + 1) * t], packed)
        sides.append(packed)
    first = me == 0
    for out, x in (
        (keep, jnp.where(first, sides[0], sides[1])),
        (send, jnp.where(first, sides[1], sides[0])),
    ):
        for u in range(plan.gram_cols):
            out[u * t : (u + 1) * t] = x[:, :, u * LANES : (u + 1) * LANES]


def quad_body(plan, *refs):
    *sums, gram, out = refs
    total = sums[0][...]
    for other in sums[1:]:
        total = total + other[...]
    out[: plan.sums] = total
    out[plan.sums :] = gram[...]


def high_body(plan, bit, mine, gram, other, out):
    for at in range(0, plan.sums, plan.high):
        for h in range(plan.high):
            out[at + h] = mine[at + h] + other[at + (h ^ bit)]
    out[plan.sums :] = gram[...] + other[plan.sums :]


def solve_body(plan, rate, *refs):
    mine, refs = refs[:QUAD][::-1], refs[QUAD:]
    theirs, refs = refs[:QUAD][::-1], refs[QUAD:]
    turned, weights, weights_out, residual_out, res0, res1, weights_new, residual, sems = refs
    each, high = plan.each, plan.high
    half = each // 2
    me = lax.axis_index("row")
    for q, h, crossed in plan.blocks():
        to = pl.ds(pl.multiple_of(chip_at(q, h) * each, each), each)
        for c in range(plan.col_tiles):
            at = c * high + h
            cols = slice(c * LANES, (c + 1) * LANES)
            res0[to, cols], res1[to, cols] = by_batch(me == crossed, mine[q][at], theirs[q][at])
    grams = lambda packet: packet[plan.sums :]
    here = grams(mine[0]) + grams(theirs[1]) + grams(theirs[2]) + grams(theirs[3])
    there = grams(theirs[0]) + grams(mine[1]) + grams(mine[2]) + grams(mine[3])
    first = me == 0
    t = plan.gram_rows
    rows = []
    for x in (jnp.where(first, here, there), jnp.where(first, there, here)):
        x = jnp.concatenate([x[u * t : (u + 1) * t] for u in range(plan.gram_cols)], 2)
        lane = lax.broadcasted_iota(jnp.int32, x.shape, 2) // plan.width
        rows += [jnp.where(lane == i, x, 0.0) for i in range(plan.pack)]
    gram = jnp.concatenate(rows, 0)
    gram = gram.reshape(-1, gram.shape[2])
    step = dot(gram, jnp.concatenate([res0[...]] * plan.pack, 0), ((1,), (0,))) * rate
    core0, core1 = (
        x.reshape(plan.chips // 2, each, -1) for x in (step[: plan.width // 2], step[plan.width // 2 :])
    )
    low = lax.broadcasted_iota(jnp.int32, core0.shape, 1) < half
    even = jnp.where(low, core0, pltpu.roll(core1, half, 1))
    odd = jnp.where(low, pltpu.roll(core0, half, 1), core1)
    res1[...] = res1[...] - jnp.stack([even, odd], 1).reshape(res1.shape)
    tile = res1[pl.ds(pl.multiple_of(lax.axis_index("center") * each, each), each), :]
    residual[...] = jnp.where(first, tile[:half], tile[half:])
    copies = [
        pltpu.make_async_copy(a, b, sems.at[i])
        for i, (a, b) in enumerate(((residual, residual_out), (weights_new, weights_out)))
    ]
    copies[0].start()
    cols = weights.shape[1]
    side = lambda x: jnp.where(first, x[:, :cols], x[:, cols:])
    both = jnp.concatenate([side(res0[...]), side(res1[...])], 0)
    grad = dot(turned[...], both, ((1,), (0,)))
    weights_new[...] = weights[...] - rate * grad
    copies[1].start()
    for c in copies:
        c.wait()


def body(dataset, centers, weights, batch_index, targets, gamma):
    shards = lax.axis_size("center")
    cores = lax.axis_size("row")
    batches, rows_here = batch_index.shape
    assert cores == 2 and batches == 2 and shards % QUAD == 0 and shards & (shards - 1) == 0
    features = dataset.shape[1]
    count, cols = weights.shape
    each = batches * rows_here
    high = shards // QUAD
    span = high * each
    n = shards * each
    width = shards * cores * rows_here
    rate = 0.5 / width
    plan = Plan(high, each, 2 * cols // LANES, width, max(1, LANES // width))
    quad = range(1, QUAD)
    bits = [1 << i for i in range(high.bit_length() - 1)]

    (local,) = call(
        pick_body,
        [kept(each, features)],
        (batch_index, pl.ANY),
        (dataset, pl.ANY),
        scratch_shapes=[
            pltpu.SMEM(batch_index.shape, jnp.int32),
            pltpu.VMEM(dataset.shape, jnp.float32),
            pltpu.SemaphoreType.DMA((2,)),
        ],
    )
    split, row = call(
        prepare_body,
        [pltpu.VMEM((3, count, features), jnp.bfloat16), kept(8, count)],
        (centers, pl.ANY),
        scratch_shapes=[pltpu.VMEM(centers.shape, jnp.float32), pltpu.SemaphoreType.DMA],
    )
    spread = jnp.broadcast_to(gamma, (8, count))
    (weight_split,) = call(
        weights_body, [pltpu.VMEM((3, count, 2 * cols), jnp.bfloat16)], weights, swap_cores(weights)
    )
    rows = local
    for bit in bits:
        rows = jnp.concatenate([rows, across(rows, QUAD * bit)], 0)
    received = [rows] + [across(rows, q) for q in quad]
    own, packets = [None] * QUAD, [None] * QUAD
    for group in ((0,), (3, 2, 1)):
        done = call(
            functools.partial(block_body, plan, len(group)),
            [kept(span, count)] * len(group)
            + [kept(plan.sums, each, LANES)] * len(group),
            spread,
            split,
            row,
            weight_split,
            *[received[q] for q in group],
            *([targets] if group == (0,) else []),
        )
        for i, q in enumerate(group):
            own[q], packets[q] = done[i], done[len(group) + i]
    sums = [across(packets[q], q) for q in reversed(quad)]
    own = jnp.concatenate(own, 0)
    turned, gram, gram_sent = call(
        functools.partial(gram_body, plan),
        [kept(count, 2 * n)] + [kept(plan.grams, each, LANES)] * 2,
        own,
        swap_cores(own),
        scratch_shapes=[pltpu.VMEM((n, count), jnp.float32)] * 2,
    )
    shape = kept(plan.tiles, each, LANES)
    (total,) = call(functools.partial(quad_body, plan), [shape], packets[0], *sums, gram_sent)
    for i, bit in enumerate(bits):
        if i == 0:
            other = across(total, QUAD * bit)
        else:
            gram = total[plan.sums :]
            other = jnp.concatenate(
                [across(total[: plan.sums], QUAD * bit), partner(gram, QUAD * bit)], 0
            )
        (total,) = call(functools.partial(high_body, plan, bit), [shape], total, gram, other)
    mine = [across(total, q) for q in reversed(quad)] + [total]
    new_weights, residual = call(
        functools.partial(solve_body, plan, rate),
        [stored(count, cols), stored(rows_here, 2 * cols)],
        *mine,
        *[swap_cores(x) for x in mine],
        turned,
        weights,
        out_space=pl.ANY,
        scratch_shapes=[
            pltpu.VMEM((width, 2 * cols), jnp.float32),
            pltpu.VMEM((width, 2 * cols), jnp.float32),
            pltpu.VMEM((count, cols), jnp.float32),
            pltpu.VMEM((rows_here, 2 * cols), jnp.float32),
            pltpu.SemaphoreType.DMA((2,)),
        ],
    )
    return (new_weights, residual)


def solution(mesh):
    return jax.shard_map(
        body,
        mesh=mesh,
        in_specs=(
            P(("groups", "center", "row"), None),
            P(("groups", "center"), None),
            P(("groups", "center"), "row"),
            P(None, ("groups", "center", "row")),
            P(None, ("groups", "center", "row"), None),
            P("groups"),
        ),
        out_specs=(P(("groups", "center"), "row"), P(("groups", "center", "row"), None)),
        check_vma=False,
    )
```
